32 devices in a mesh: dp: 8 (over y, x, core), head: 4 (over z).
Axes of the slice: x: 2, y: 2, z: 4, core: 2. Of those that a mesh axis runs over, the one named last changes fastest.
Arguments:
- tokens: bfloat16 [2048, 2048], P('dp', 'head'), may hold values from -6 to 6
- mixer_gain: float32 [2048], replicated, may hold values from 0.1 to 1.9
- query_weight: bfloat16 [2048, 1024], P(None, 'head'), may hold values from -0.125 to 0.125
- key_weight: bfloat16 [3, 2048, 1024], P(None, None, 'head'), may hold values from -0.125 to 0.125
- value_weight: bfloat16 [3, 2048, 1024], P(None, None, 'head'), may hold values from -0.125 to 0.125
- beta_weight: bfloat16 [2048, 24], P(None, 'head'), may hold values from -0.125 to 0.125
- head_gain: float32 [128], replicated, may hold values from 0.1 to 1.9
- output_weight: bfloat16 [1024, 2048], P('head'), may hold values from -0.1875 to 0.1875
- expert_gain: float32 [2048], replicated, may hold values from 0.1 to 1.9
- router_weight: float32 [2048, 16], replicated, may hold values from -0.125 to 0.125
- expert_ids: int32 [2048, 2], P(('dp', 'head')), may hold values from 0 to 15, all different within a row; in each aligned block of 64 rows (0 to 63, 64 to 127, ...) at most 16 rows name the same one
- gate_weight: bfloat16 [16, 2048, 1408], P('dp'), may hold values from -0.125 to 0.125
- up_weight: bfloat16 [16, 2048, 1408], P('dp'), may hold values from -0.125 to 0.125
- down_weight: bfloat16 [16, 1408, 2048], P('dp'), may hold values from -0.15625 to 0.15625
Outputs:
- layer_out: bfloat16 [2048, 2048], P(('dp', 'head'))
The draws below stay inside these ranges and needn't reach their ends.
Inputs may be any that keep to these rules, and one draw needn't show every extreme that they name: `expert_ids`: taking the tokens in aligned blocks of 64 (the rows of one device), no expert is named by more than 16 rows of a block, a bound that some block reaches; a token's two experts differ.
All inputs are finite; a program needn't handle non-finite values.
Results may differ from the reference program's by a relative error of at most 0.012.
Values may be sent and summed in bfloat16 or wider, within the bound.
A program may use at most 128 MiB of HBM per device.

```python
import math
import jax
import jax.numpy as jnp
import numpy as np
from jax import lax

D = 2048
HEADS = 8
DK = 128
NH = 3
FFE = 1408
TOK_DEV = 256
TOKENS = 2048
ROWS = 64
EXPERTS = 16
CAP = 16
N_DP = 8
N_HEAD = 4


def level_of(own_key, shape, shards, smallest, high):
    loudness, own = 1.0, jax.random.fold_in(own_key, 6)
    for dim, parts in shards:
        heights = jnp.exp(jax.random.uniform(jax.random.fold_in(own, dim), (parts,), jnp.float32, smallest / len(shards), high / len(shards)))
        loudness = loudness * jnp.repeat(heights, shape[dim] // parts).reshape([-1 if axis == dim else 1 for axis in range(len(shape))])
    return loudness


def deal_out(rng, own, number, rows, number_of, top, reach, skew):
    ranking = jax.random.permutation(rng, number_of)
    packed, common = load_shares(number_of, rows * top, reach, skew, True), load_shares(number_of, rows * top, reach, skew, False)
    places = jnp.arange(number_of)

    def named(tallies, rotation):
        used = int((tallies > 0).sum())
        fixed = max(1, used // 4)
        moved = fixed + (places - fixed + rotation * (used - fixed)) % max(1, number_of - fixed)
        return jnp.zeros((number_of,), jnp.int32).at[ranking[jnp.where(places < fixed, places, moved)]].set(jnp.asarray(tallies, jnp.int32))

    tallies = jnp.where(number % 4 == 0, named(packed, number // 4), named(common, number - number // 4 - 1))
    mixed = jax.random.permutation(jax.random.fold_in(own, 3), number_of)
    giver, sink = mixed[0:number_of // 2 * 2:2], mixed[1:number_of // 2 * 2:2]
    slack = jnp.minimum(tallies[giver] - 1, reach - tallies[sink]) // 2
    slack = jnp.where((giver == ranking[0]) | (sink == ranking[0]) | (tallies[sink] == 0), 0, jnp.maximum(slack, 0))
    moved = jax.random.randint(jax.random.fold_in(own, 4), (number_of // 2,), 0, 1 << 20) % (slack + 1)
    tallies = tallies.at[giver].add(-moved).at[sink].add(moved)
    labels = jnp.searchsorted(jnp.cumsum(tallies), jnp.arange(rows * top), side="right").astype(jnp.int32)
    listing = labels.reshape(top, rows).T
    listing = listing[jax.random.permutation(jax.random.fold_in(own, 1), rows)]
    rotation = jax.random.randint(jax.random.fold_in(own, 2), (rows, 1), 0, top)
    return jnp.take_along_axis(listing, (jnp.arange(top)[None, :] + rotation) % top, axis=1)


def load_shares(number_of, total, limit, lean, full):
    loads = [(1 << 20) // math.isqrt(standing ** lean) + 1 for standing in range(1, number_of + 1)]
    largest = limit if full else min(limit, max(-(-total // number_of), total * loads[0] // sum(loads)))
    least = 1 if total - largest >= number_of - 1 else 0
    holding, spare = [largest] + [least] * (number_of - 1), total - largest - least * (number_of - 1)
    while spare > 0:
        movable = [i for i in range(1, number_of) if holding[i] < largest] or [i for i in range(1, number_of) if holding[i] < limit]
        mass, remaining = sum([loads[i] for i in movable]), spare
        for i in movable:
            more = min(limit - holding[i], max(1, remaining * loads[i] // mass), spare)
            holding[i] = holding[i] + more
            spare = spare - more
    return np.array(holding)


def noise(key, shape, width, most, cuts=(), held_as=jnp.bfloat16):
    loudness = level_of(key, shape, cuts, -0.22, 0.18) if cuts else 1.0
    entries = jax.random.normal(key, shape, jnp.float32) * width * loudness
    return jnp.minimum(jnp.maximum(entries, -most), most).astype(held_as)


def setup_inputs(seed: int = 0) -> dict:
    streams_of = jax.random.split(jax.random.key(seed), 15)
    tokens = noise(streams_of[0], (TOKENS, D), 1.0, 6.0, ((0, 8), (1, 4)))
    mixer_gain = jnp.clip(1.0 + 0.18 * jax.random.normal(streams_of[1], (D,), jnp.float32), 0.1, 1.9)
    query_weight = noise(streams_of[2], (D, HEADS * DK), D ** -0.5, 0.125, ((1, 4),))
    key_weight = noise(streams_of[3], (NH, D, HEADS * DK), D ** -0.5, 0.125, ((2, 4),))
    value_weight = noise(streams_of[4], (NH, D, HEADS * DK), D ** -0.5, 0.125, ((2, 4),))
    beta_weight = noise(streams_of[5], (D, HEADS * NH), D ** -0.5, 0.125, ((1, 4),))
    head_gain = jnp.clip(1.0 + 0.18 * jax.random.normal(streams_of[6], (DK,), jnp.float32), 0.1, 1.9)
    output_weight = noise(streams_of[7], (HEADS * DK, D), (HEADS * DK) ** -0.5, 0.1875, ((0, 4),))
    expert_gain = jnp.clip(1.0 + 0.18 * jax.random.normal(streams_of[8], (D,), jnp.float32), 0.1, 1.9)
    router_weight = noise(streams_of[9], (D, EXPERTS), D ** -0.5, 0.125, (), jnp.float32)
    expert_ids_keys = jax.random.split(jax.random.fold_in(streams_of[10], 1), TOKENS // ROWS)
    expert_ids_turns = jax.random.permutation(jax.random.fold_in(streams_of[10], 3), TOKENS // ROWS)
    expert_ids = jax.vmap(lambda own, number: deal_out(jax.random.fold_in(streams_of[10], 2), own, number, ROWS, EXPERTS, 2, CAP, 2))(expert_ids_keys, expert_ids_turns).reshape((TOKENS, 2))
    gate_weight = noise(streams_of[11], (EXPERTS, D, FFE), D ** -0.5, 0.125, ((0, 8),))
    up_weight = noise(streams_of[12], (EXPERTS, D, FFE), D ** -0.5, 0.125, ((0, 8),))
    down_weight = noise(streams_of[13], (EXPERTS, FFE, D), FFE ** -0.5, 0.15625, ((0, 8),))
    return dict(tokens=tokens, mixer_gain=mixer_gain, query_weight=query_weight, key_weight=key_weight, value_weight=value_weight, beta_weight=beta_weight, head_gain=head_gain, output_weight=output_weight, expert_gain=expert_gain, router_weight=router_weight, expert_ids=expert_ids, gate_weight=gate_weight, up_weight=up_weight, down_weight=down_weight)


EPSILON = 1e-06
TOP_PRECISION = lax.Precision.HIGHEST

def root_norm(values, gain):
    return values * lax.rsqrt(lax.optimization_barrier(jnp.mean(values * values, -1, keepdims=True)) + EPSILON) * gain

def unit_vector(values):
    return values * lax.rsqrt(lax.optimization_barrier(jnp.sum(values * values, -1, keepdims=True)) + EPSILON)

def reference(tokens, mixer_gain, query_weight, key_weight, value_weight, beta_weight, head_gain, output_weight, expert_gain, router_weight, expert_ids, gate_weight, up_weight, down_weight):
    widened = tokens.astype(jnp.float32)
    normed = root_norm(widened, mixer_gain).astype(jnp.bfloat16)
    query = unit_vector(jnp.dot(normed, query_weight, preferred_element_type=jnp.float32).reshape(TOKENS, HEADS, DK)) * DK ** (-0.5)
    key_rows = unit_vector(jnp.stack([jnp.dot(normed, key_weight[member], preferred_element_type=jnp.float32) for member in range(NH)], 1).reshape(TOKENS, NH, HEADS, DK))
    value_rows = jnp.stack([jnp.dot(normed, value_weight[member], preferred_element_type=jnp.float32) for member in range(NH)], 1).reshape(TOKENS, NH, HEADS, DK)
    beta_rows = 2.0 * jax.nn.sigmoid(jnp.dot(normed, beta_weight, preferred_element_type=jnp.float32))
    beta_rows = jnp.transpose(beta_rows.reshape(TOKENS, HEADS, NH), (0, 2, 1))
    sequences = (jnp.transpose(query.reshape(N_DP, TOK_DEV, HEADS, DK), (1, 0, 2, 3)), jnp.transpose(key_rows.reshape(N_DP, TOK_DEV, NH, HEADS, DK), (1, 2, 0, 3, 4)), jnp.transpose(value_rows.reshape(N_DP, TOK_DEV, NH, HEADS, DK), (1, 2, 0, 3, 4)), jnp.transpose(beta_rows.reshape(N_DP, TOK_DEV, NH, HEADS), (1, 2, 0, 3)))

    def advance(memory_state, inputs):
        query_now, keys_now, values_now, betas_now = inputs
        for member in range(NH):
            predicted = jnp.einsum('bhkv,bhk->bhv', memory_state, keys_now[member], precision=TOP_PRECISION)
            update = betas_now[member][..., None] * (values_now[member] - predicted)
            memory_state = memory_state + keys_now[member][..., :, None] * update[..., None, :]
        return (memory_state, jnp.einsum('bhkv,bhk->bhv', memory_state, query_now, precision=TOP_PRECISION))
    start_memory = jnp.zeros((N_DP, HEADS, DK, DK), jnp.float32)
    mixed_heads = lax.scan(advance, start_memory, sequences)[1]
    mixed_heads = jnp.transpose(mixed_heads, (1, 0, 2, 3)).reshape(TOKENS, HEADS, DK)
    head_out = root_norm(mixed_heads, head_gain).astype(jnp.bfloat16).reshape(TOKENS, HEADS * DK)
    residual = widened + jnp.dot(head_out, output_weight, preferred_element_type=jnp.float32)
    routed = root_norm(residual, expert_gain)
    logits = jnp.dot(routed, router_weight, precision=TOP_PRECISION)
    choose = expert_ids[:, :, None] == jnp.arange(EXPERTS, dtype=jnp.int32)[None, None, :]
    chosen = lax.optimization_barrier(jnp.sum(jnp.where(choose, logits[:, None, :], 0.0), -1))
    leading = jax.nn.sigmoid(chosen[:, 0] - chosen[:, 1])
    pair_weight = jnp.stack([leading, 1.0 - leading], 1)
    block_count = N_DP * N_HEAD
    flat_ids = expert_ids.reshape(block_count, 2 * ROWS).astype(jnp.int32)
    one_hot = (flat_ids[:, :, None] == jnp.arange(EXPERTS, dtype=jnp.int32)[None, None, :]).astype(jnp.int32)
    position = lax.optimization_barrier(jnp.sum((jnp.cumsum(one_hot, 1) - one_hot) * one_hot, 2)).astype(jnp.int32)
    source = jnp.arange(block_count, dtype=jnp.int32)[:, None]
    target = (flat_ids * (block_count * CAP) + source * CAP + position).reshape(-1).astype(jnp.int32)
    expert_rows = routed.astype(jnp.bfloat16)
    buffer_rows = jnp.zeros((EXPERTS * block_count * CAP, D), jnp.bfloat16).at[target].set(jnp.repeat(expert_rows, 2, 0))
    buffer_rows = buffer_rows.reshape(EXPERTS, block_count * CAP, D)

    def one_expert(pieces):
        arrived, gate_part, up_part, down_part = pieces
        gate_rows = jnp.dot(arrived, gate_part, preferred_element_type=jnp.float32)
        lifted = jnp.dot(arrived, up_part, preferred_element_type=jnp.float32)
        hidden = (jax.nn.silu(gate_rows) * lifted).astype(jnp.bfloat16)
        return jnp.dot(hidden, down_part, preferred_element_type=jnp.float32).astype(jnp.bfloat16)
    produced = lax.map(one_expert, (buffer_rows, gate_weight, up_weight, down_weight))
    picked = produced.reshape(EXPERTS * block_count * CAP, D)[target].reshape(TOKENS, 2, D)
    blended = lax.optimization_barrier(jnp.sum(pair_weight[:, :, None] * picked.astype(jnp.float32), 1))
    return (residual + blended).astype(jnp.bfloat16)
```

```python
import functools

import jax
import jax.numpy as jnp
from jax import lax
from jax.experimental import pallas as pl
from jax.experimental.pallas import tpu as pltpu
from jax.sharding import PartitionSpec as P

DK = 128
NH = 3
CT = 32
DIRECT = 0
AHEAD = 3
RELAY_STEPS = 4


EPSILON = 1e-06
TOP_PRECISION = lax.Precision.HIGHEST
MESH = pl.DeviceIdType.MESH
VMEM = pl.BlockSpec(memory_space=pltpu.VMEM)
ANY = pl.BlockSpec(memory_space=pl.ANY)
HBM = pl.BlockSpec(memory_space=pltpu.HBM)
F32 = jnp.float32
BF16 = jnp.bfloat16


def root_norm(values, gain):
    return values * lax.rsqrt(jnp.mean(values * values, -1, keepdims=True) + EPSILON) * gain


def greet(axis, peers):
    barrier = pltpu.get_barrier_semaphore()
    for peer in peers:
        pl.semaphore_signal(barrier, inc=1, device_id={axis: peer}, device_id_type=MESH)
    pl.semaphore_wait(barrier, len(peers))


def remote(src, dst, send, recv, slot, axis, peer):
    return pltpu.make_async_remote_copy(
        src_ref=src,
        dst_ref=dst,
        send_sem=send.at[slot],
        recv_sem=recv.at[slot],
        device_id={axis: peer},
        device_id_type=MESH,
    )


def ring_scatter_kernel(
    axis, n, x_ref, from_left, from_right, pass_l, pass_r, sum_l, sum_r, send, recv
):
    me = lax.axis_index(axis)
    right, left = lax.rem(me + 1, n), lax.rem(me + n - 1, n)
    far = lax.rem(me + 2, n)
    half = x_ref.shape[1] // 2
    top, low = pl.ds(0, half), pl.ds(half, half)
    greet(axis, (left, right))
    first = remote(x_ref.at[far, top], pass_l, send, recv, 0, axis, right)
    second = remote(x_ref.at[far, low], pass_r, send, recv, 1, axis, left)
    third = remote(x_ref.at[right, low], from_left.at[low], send, recv, 2, axis, right)
    fourth = remote(x_ref.at[left, top], from_right.at[top], send, recv, 3, axis, left)
    first.start()
    second.start()
    third.start()
    fourth.start()
    first.wait_recv()
    sum_l[...] = (pass_l[...].astype(F32) + x_ref[right, top].astype(F32)).astype(BF16)
    fifth = remote(sum_l, from_left.at[top], send, recv, 4, axis, right)
    fifth.start()
    second.wait_recv()
    sum_r[...] = (pass_r[...].astype(F32) + x_ref[left, low].astype(F32)).astype(BF16)
    sixth = remote(sum_r, from_right.at[low], send, recv, 5, axis, left)
    sixth.start()
    first.wait_send()
    second.wait_send()
    third.wait()
    fourth.wait()
    fifth.wait()
    sixth.wait()


def ring_scatter(parts, axis, n):
    rows, width = parts.shape[1:]
    if n != 4:
        return lax.psum_scatter(parts, axis, scatter_dimension=0, tiled=False).astype(F32)
    block = jax.ShapeDtypeStruct((rows, width), parts.dtype)
    from_left, from_right = pl.pallas_call(
        functools.partial(ring_scatter_kernel, axis, n),
        out_shape=(block, block),
        in_specs=[VMEM],
        out_specs=(VMEM, VMEM),
        scratch_shapes=[pltpu.VMEM((rows // 2, width), parts.dtype)] * 4
        + [pltpu.SemaphoreType.DMA((6,)), pltpu.SemaphoreType.DMA((6,))],
        compiler_params=pltpu.CompilerParams(
            collective_id=1, has_side_effects=True, vmem_limit_bytes=8 << 20
        ),
        cost_estimate=pl.CostEstimate(flops=0, bytes_accessed=20 << 20, transcendentals=0),
        name="ring_scatter",
    )(parts)
    own = lax.dynamic_index_in_dim(parts, lax.axis_index(axis), 0, keepdims=False)
    return own.astype(F32) + (from_left.astype(F32) + from_right.astype(F32))


def experts_kernel(
    axis,
    n,
    x_ref,
    gate_ref,
    up_ref,
    down_ref,
    out_ref,
    gate_buf,
    up_buf,
    down_buf,
    arrived_ref,
    result_ref,
    load_sem,
    send,
    recv,
    back_send,
    back_recv,
    own_sem,
):
    me = lax.axis_index(axis)
    experts, capacity = gate_ref.shape[0], x_ref.shape[1] // gate_ref.shape[0]
    width = x_ref.shape[2]
    loads = []
    for e in range(experts):
        row = []
        for i, (source, target) in enumerate(
            ((gate_ref, gate_buf), (up_ref, up_buf), (down_ref, down_buf))
        ):
            row.append(pltpu.make_async_copy(source.at[e], target.at[e], load_sem.at[e, i]))
            row[-1].start()
        loads.append(row)
    steps = range(n - 1, 0, -1)
    peers = {step: lax.rem(me + step, n) for step in steps}
    greet(axis, [peers[step] for step in steps])
    copies = []
    for step in steps:
        peer = peers[step]
        copies.append(
            remote(x_ref.at[peer], arrived_ref.at[me], send, recv, step, axis, peer)
        )
        copies[-1].start()
    own = pltpu.make_async_copy(x_ref.at[me], arrived_ref.at[me], own_sem)
    own.start()
    own.wait()
    for copy in copies:
        copy.wait()
    returns = []
    for e in range(experts):
        span = pl.ds(e * capacity, capacity)
        rows = jnp.concatenate([arrived_ref[s, span] for s in range(n)], 0)
        loads[e][0].wait()
        gated = jnp.dot(rows, gate_buf[e], preferred_element_type=F32)
        loads[e][1].wait()
        lifted = jnp.dot(rows, up_buf[e], preferred_element_type=F32)
        hidden = (gated / (1.0 + jnp.exp(-gated)) * lifted).astype(BF16)
        loads[e][2].wait()
        made = jnp.dot(hidden, down_buf[e], preferred_element_type=F32).astype(BF16)
        for s in range(n):
            result_ref[s, span] = made[s * capacity : (s + 1) * capacity]
        for step in steps:
            peer = peers[step]
            slot = e * n + step
            returns.append(
                remote(
                    result_ref.at[peer, span],
                    out_ref.at[me, span],
                    back_send,
                    back_recv,
                    slot,
                    axis,
                    peer,
                )
            )
            returns[-1].start()
    own = pltpu.make_async_copy(result_ref.at[me], out_ref.at[me], own_sem)
    own.start()
    own.wait()
    for copy in returns:
        copy.wait()


def run_experts(x, gate, up, down, axis, n):
    experts = gate.shape[0]
    return pl.pallas_call(
        functools.partial(experts_kernel, axis, n),
        out_shape=jax.ShapeDtypeStruct(x.shape, x.dtype),
        in_specs=[VMEM, ANY, ANY, ANY],
        out_specs=VMEM,
        scratch_shapes=[
            pltpu.VMEM(gate.shape, gate.dtype),
            pltpu.VMEM(up.shape, up.dtype),
            pltpu.VMEM(down.shape, down.dtype),
            pltpu.VMEM(x.shape, x.dtype),
            pltpu.VMEM(x.shape, x.dtype),
            pltpu.SemaphoreType.DMA((experts, 3)),
            pltpu.SemaphoreType.DMA((n,)),
            pltpu.SemaphoreType.DMA((n,)),
            pltpu.SemaphoreType.DMA((experts * n,)),
            pltpu.SemaphoreType.DMA((experts * n,)),
            pltpu.SemaphoreType.DMA,
        ],
        compiler_params=pltpu.CompilerParams(collective_id=2, has_side_effects=True, vmem_limit_bytes=48 << 20),
        cost_estimate=pl.CostEstimate(
            flops=5 << 30, bytes_accessed=50 << 20, transcendentals=0
        ),
        name="experts",
    )(x, gate, up, down)


NN = (((1,), (0,)), ((), ()))
NT = (((1,), (1,)), ((), ()))
TN = (((0,), (0,)), ((), ()))


def dot1(a, b, dims=NN):
    return lax.dot_general(a.astype(BF16), b.astype(BF16), dims, preferred_element_type=F32)


def halves(a):
    high = a.astype(BF16)
    return high, (a - high.astype(F32)).astype(BF16)


def dot3(a, b, dims=NN):
    ah, al = a
    bh, bl = b
    product = functools.partial(
        lax.dot_general, dimension_numbers=dims, preferred_element_type=F32
    )
    return product(ah, bh) + (product(ah, bl) + product(al, bh))


def chunk_mixer_kernel(
    axis,
    n,
    heads,
    x_in,
    gain_in,
    qw_in,
    kw_in,
    vw_in,
    bw_in,
    head_gain_in,
    ow_in,
    out_ref,
    mine_ref,
    blocks_ref,
    normed_ref,
    state_ref,
    gain_ref,
    qw_ref,
    kw_ref,
    vw_ref,
    bw_ref,
    head_gain_ref,
    ow_ref,
    load_sem,
    own_sem,
    send,
    recv,
    relay_send,
):
    me = lax.axis_index(axis)
    length, width = x_in.shape
    rows = length // n
    chunks = length // rows
    subs = rows // CT
    own = pltpu.make_async_copy(x_in, blocks_ref.at[me], own_sem)
    own.start()
    loads = [
        (gain_in, gain_ref),
        (kw_in, kw_ref),
        (vw_in, vw_ref),
        (qw_in, qw_ref),
        (bw_in, bw_ref),
        (head_gain_in, head_gain_ref),
        (ow_in, ow_ref),
    ]
    loads = [
        pltpu.make_async_copy(source, target, load_sem.at[i])
        for i, (source, target) in enumerate(loads)
    ]
    for load in loads:
        load.start()
    greet(axis, [lax.rem(me + step, n) for step in range(1, n)])
    own.wait()

    def piece(s, c):
        return blocks_ref.at[s, pl.ds(pl.multiple_of(c * rows, rows), rows)]

    def carry(s, c, send_sem, peer):
        return pltpu.make_async_remote_copy(
            src_ref=piece(s, c),
            dst_ref=piece(s, c),
            send_sem=send_sem,
            recv_sem=recv.at[s, c],
            device_id={axis: peer},
            device_id_type=MESH,
        )

    def own_sends(c, action):
        for step in range(1, n):
            upward, downward = me + step < n, me >= step
            if n == 4 and 1 < step < RELAY_STEPS:
                straight = c < DIRECT
                upward = upward & (straight | (me + step < n - 1))
                downward = downward & (straight | (me > step))

            @pl.when(upward)
            def _():
                action(carry(me, c, send.at[c, step, 0], lax.rem(me + step, n)))

            @pl.when(downward)
            def _():
                action(carry(me, c, send.at[c, step, 1], lax.rem(me + n - step, n)))

    def relays(s, c, action):
        middle = n - 2 if s < n // 2 else 1

        @pl.when((me == middle) & (c >= DIRECT))
        def _():
            action(carry(s, c, relay_send.at[s, c], 0 if s >= n // 2 else n - 1))

    for c in range(min(AHEAD, chunks)):
        own_sends(c, lambda copy: copy.start())
    order = sorted(range(n), key=lambda s: abs(2 * s - (n - 1)))

    for h in range(heads):
        state_ref[h] = jnp.zeros((DK, DK), F32)
    for load in loads:
        load.wait()

    rows_c = NH * CT
    later = lax.broadcasted_iota(jnp.int32, (rows_c, rows_c), 0)
    early = lax.broadcasted_iota(jnp.int32, (rows_c, rows_c), 1)
    later_t, early_t = later % CT, early % CT
    same_token = later_t == early_t
    strict = (early_t < later_t) | (same_token & (early < later))
    eye = (later == early).astype(F32)
    seen = (lax.broadcasted_iota(jnp.int32, (CT, rows_c), 1) % CT) <= lax.broadcasted_iota(
        jnp.int32, (CT, rows_c), 0
    )

    def unit(values):
        return values * lax.rsqrt(jnp.sum(values * values, -1, keepdims=True) + EPSILON)

    def head_of(values, h):
        return values[:, h * DK : (h + 1) * DK]

    def step_chunk(c, _):
        if AHEAD < chunks:

            @pl.when(c + AHEAD < chunks)
            def _():
                own_sends(c + AHEAD, lambda copy: copy.start())

        for s in order:

            @pl.when(me != s)
            def _():
                carry(s, c, send.at[0, 0, 0], lax.rem(me + 1, n)).wait_recv()

            if n == 4 and (RELAY_STEPS > 3 or 0 < s < n - 1):
                relays(s, c, lambda copy: copy.start())
        span = pl.ds(pl.multiple_of(c * rows, rows), rows)
        square = jnp.zeros((rows, 1), F32)
        for s in range(n):
            part = blocks_ref[s, span].astype(F32)
            square = square + jnp.sum(part * part, -1, keepdims=True)
        scale = lax.rsqrt(square / (n * width) + EPSILON)
        for s in range(n):
            cols = pl.ds(s * width, width)
            normed_ref[:, cols] = (
                blocks_ref[s, span].astype(F32) * scale * gain_ref[:, cols]
            ).astype(BF16)

        def project(weight):
            return jnp.dot(normed_ref[...], weight, preferred_element_type=F32)

        key_parts = [project(kw_ref[m]) for m in range(NH)]
        beta = 2.0 / (
            1.0
            + jnp.exp(
                -lax.dot_general(normed_ref[...], bw_ref[...], NT, preferred_element_type=F32)
            )
        )

        def rows_of(member_parts, j):
            return jnp.concatenate(
                [part[j * CT : (j + 1) * CT] for part in member_parts], 0
            )

        cases = [(h, j) for h in range(heads) for j in range(subs)]
        units = [[unit(head_of(part, h)) for part in key_parts] for h in range(heads)]
        all_keys, all_scaled, betas, parts = [], [], [], []
        for h, j in cases:
            keys = rows_of(units[h], j)
            betas.append(
                rows_of([beta[:, h * NH + m : h * NH + m + 1] for m in range(NH)], j)
            )
            scaled = keys * betas[-1]
            all_scaled.append(scaled)
            all_keys.append(halves(keys))
            similar = dot3(halves(scaled), all_keys[-1], NT)
            parts.append(jnp.where(strict, similar, 0.0))
        inverses = []
        for part in parts:
            inner = jnp.where(same_token, part, 0.0)
            inverses.append(eye - inner + dot1(inner, inner))
        side = [lambda m=m: project(vw_ref[m]) for m in range(NH)]
        side.append(lambda: project(qw_ref[...]))
        side_parts = []
        size = 1
        while size < CT:
            joined = (later_t // (2 * size) == early_t // (2 * size)) & (
                later_t // size != early_t // size
            )
            steps = [
                dot1(jnp.where(joined, part, 0.0), inverse)
                for part, inverse in zip(parts, inverses)
            ]
            if side:
                side_parts.append(side.pop(0)())
            inverses = [
                inverse - dot1(inverse, step) for inverse, step in zip(inverses, steps)
            ]
            size *= 2
        while side:
            side_parts.append(side.pop(0)())
        value_parts, query_part = side_parts[:NH], side_parts[NH]
        queries = [
            halves(unit(head_of(query_part, h))[j * CT : (j + 1) * CT] * DK ** (-0.5))
            for h, j in cases
        ]
        rights = [
            jnp.concatenate(
                [scaled, rows_of([head_of(part, h) for part in value_parts], j) * betas_now], 1
            )
            for (h, j), scaled, betas_now in zip(cases, all_scaled, betas)
        ]
        guesses = [dot1(inverse, right) for inverse, right in zip(inverses, rights)]
        attends = [
            halves(jnp.where(seen, dot3(query, keys, NT), 0.0))
            for query, keys in zip(queries, all_keys)
        ]
        rests = [
            right - guess - dot3(halves(part), halves(guess))
            for right, guess, part in zip(rights, guesses, parts)
        ]
        all_solved = [
            guess + dot1(inverse, rest)
            for guess, inverse, rest in zip(guesses, inverses, rests)
        ]
        befores = [state_ref[h] for h in range(heads)]
        mixes = [[] for _ in range(heads)]
        for j in range(subs):
            for h in range(heads):
                i = h * subs + j
                state = halves(befores[h])
                solved = all_solved[i]
                corrected = solved[:, DK:] - dot3(halves(solved[:, :DK]), state)
                split = halves(corrected)
                mixed = dot3(queries[i], state) + dot3(attends[i], split)
                befores[h] = befores[h] + dot3(all_keys[i], split, TN)
                mixes[h].append(root_norm(mixed, head_gain_ref[...]).astype(BF16))
        for h in range(heads):
            state_ref[h] = befores[h]
        mixes = [jnp.concatenate(mix, 0) for mix in mixes]
        out_ref[c] = jnp.dot(
            jnp.concatenate(mixes, 1), ow_ref[...], preferred_element_type=F32
        ).astype(BF16)
        return 0

    lax.fori_loop(0, chunks, step_chunk, 0)
    for s in range(n):
        mine_ref[:, pl.ds(s * width, width)] = blocks_ref[
            s, pl.ds(pl.multiple_of(me * rows, rows), rows)
        ]
    for c in range(chunks):
        own_sends(c, lambda copy: copy.wait_send())
        if n == 4:
            for s in range(n) if RELAY_STEPS > 3 else range(1, n - 1):
                relays(s, c, lambda copy: copy.wait_send())


def chunk_mixer(x, mixer_gain, qw, kw, vw, bw, head_gain, ow, axis, n):
    length, width = x.shape
    heads = qw.shape[1] // DK
    model_width = n * width
    chunks = n
    bw_t = bw.T
    gain, head_gain = mixer_gain.reshape(1, -1), head_gain.reshape(1, -1)
    return pl.pallas_call(
        functools.partial(chunk_mixer_kernel, axis, n, heads),
        out_shape=(
            jax.ShapeDtypeStruct((chunks, length // n, model_width), BF16),
            jax.ShapeDtypeStruct((length // n, model_width), BF16),
        ),
        in_specs=[ANY] * 8,
        out_specs=(VMEM, VMEM),
        scratch_shapes=[
            pltpu.VMEM((n, length, width), BF16),
            pltpu.VMEM((length // n, model_width), BF16),
            pltpu.VMEM((heads, DK, DK), F32),
            pltpu.VMEM(gain.shape, F32),
            pltpu.VMEM(qw.shape, BF16),
            pltpu.VMEM(kw.shape, BF16),
            pltpu.VMEM(vw.shape, BF16),
            pltpu.VMEM(bw_t.shape, BF16),
            pltpu.VMEM(head_gain.shape, F32),
            pltpu.VMEM(ow.shape, BF16),
            pltpu.SemaphoreType.DMA((7,)),
            pltpu.SemaphoreType.DMA,
            pltpu.SemaphoreType.DMA((chunks, n, 2)),
            pltpu.SemaphoreType.DMA((n, chunks)),
            pltpu.SemaphoreType.DMA((n, chunks)),
        ],
        compiler_params=pltpu.CompilerParams(
            collective_id=0, has_side_effects=True, vmem_limit_bytes=60 << 20
        ),
        cost_estimate=pl.CostEstimate(
            flops=20 << 30, bytes_accessed=12 << 20, transcendentals=0
        ),
        name="chunk_mixer",
    )(x, gain, qw, kw, vw, bw_t, head_gain, ow)


def shards(
    heads_axis,
    owners,
    tokens,
    mixer_gain,
    query_weight,
    key_weight,
    value_weight,
    beta_weight,
    head_gain,
    output_weight,
    expert_gain,
    router_weight,
    expert_ids,
    gate_weight,
    up_weight,
    down_weight,
):
    parts, mine = chunk_mixer(
        tokens,
        mixer_gain,
        query_weight,
        key_weight,
        value_weight,
        beta_weight,
        head_gain,
        output_weight,
        "head",
        heads_axis,
    )
    own_rows, model_width = mine.shape
    parts = parts.reshape(heads_axis, own_rows, model_width)
    attended = ring_scatter(parts, "head", heads_axis)
    residual = mine.astype(F32) + attended
    routed = root_norm(residual, expert_gain)
    logits = jnp.dot(routed, router_weight, precision=TOP_PRECISION)
    experts_total = router_weight.shape[1]
    labels = jnp.arange(experts_total, dtype=jnp.int32)
    choose = expert_ids[:, :, None] == labels[None, None, :]
    chosen = jnp.sum(jnp.where(choose, logits[:, None, :], 0.0), -1)
    leading = jax.nn.sigmoid(chosen[:, 0] - chosen[:, 1])
    pair_weight = jnp.stack([leading, 1.0 - leading], 1)
    capacity = 4 * own_rows // experts_total
    slots = experts_total * capacity
    picks = jnp.sum(choose.astype(F32), 1)
    before = jnp.arange(own_rows)[:, None] > jnp.arange(own_rows)[None, :]
    earlier = jnp.dot(before.astype(BF16), picks.astype(BF16), preferred_element_type=F32)
    position = jnp.sum(jnp.where(choose, earlier[:, None, :], 0.0), -1).astype(jnp.int32)
    target = expert_ids * capacity + position
    placed = target[:, :, None] == jnp.arange(slots, dtype=jnp.int32)[None, None, :]
    spread = jnp.any(placed, 1)
    expert_rows = routed.astype(BF16)
    outgoing = lax.dot_general(
        spread.astype(BF16), expert_rows, TN, preferred_element_type=F32
    ).astype(BF16)
    outgoing = outgoing.reshape(owners, slots // owners, model_width)
    returned = run_experts(outgoing, gate_weight, up_weight, down_weight, "dp", owners)
    weights = jnp.sum(jnp.where(placed, pair_weight[:, :, None], 0.0), 1)
    weights_high = weights.astype(BF16)
    weights_low = (weights - weights_high.astype(F32)).astype(BF16)
    stacked = jnp.concatenate([weights_high, weights_low], 0)
    blended = jnp.dot(
        stacked, returned.reshape(slots, model_width), preferred_element_type=F32
    )
    blended = blended[:own_rows] + blended[own_rows:]
    return (residual + blended).astype(BF16)


def solution(mesh):
    return jax.shard_map(
        functools.partial(shards, mesh.shape["head"], mesh.shape["dp"]),
        mesh=mesh,
        in_specs=(
            P("dp", "head"),
            P(),
            P(None, "head"),
            P(None, None, "head"),
            P(None, None, "head"),
            P(None, "head"),
            P(),
            P("head", None),
            P(),
            P(),
            P(("dp", "head"), None),
            P("dp", None, None),
            P("dp", None, None),
            P("dp", None, None),
        ),
        out_specs=P(("dp", "head"), None),
        check_vma=False,
    )
```

```python
import functools

import jax
import jax.numpy as jnp
from jax import lax
from jax.experimental import pallas as pl
from jax.experimental.pallas import tpu as pltpu
from jax.sharding import PartitionSpec as P

DK = 128
NH = 3
CT = 32
DIRECT = 0
GROUPS = 4
AHEAD = 3
RELAY_STEPS = 4


EPSILON = 1e-06
TOP_PRECISION = lax.Precision.HIGHEST
MESH = pl.DeviceIdType.MESH
VMEM = pl.BlockSpec(memory_space=pltpu.VMEM)
ANY = pl.BlockSpec(memory_space=pl.ANY)
HBM = pl.BlockSpec(memory_space=pltpu.HBM)
F32 = jnp.float32
BF16 = jnp.bfloat16


def root_norm(values, gain):
    return values * lax.rsqrt(jnp.mean(values * values, -1, keepdims=True) + EPSILON) * gain


NN = (((1,), (0,)), ((), ()))
NT = (((1,), (1,)), ((), ()))
TN = (((0,), (0,)), ((), ()))


def dot1(a, b, dims=NN):
    return lax.dot_general(a.astype(BF16), b.astype(BF16), dims, preferred_element_type=F32)


def halves(a):
    high = a.astype(BF16)
    return high, (a - high.astype(F32)).astype(BF16)


def dot3(a, b, dims=NN):
    ah, al = a
    bh, bl = b
    product = functools.partial(
        lax.dot_general, dimension_numbers=dims, preferred_element_type=F32
    )
    return product(ah, bh) + (product(ah, bl) + product(al, bh))


def layer_kernel(
    axis,
    n,
    heads,
    owners_axis,
    owners,
    x_in,
    gain_in,
    qw_in,
    kw_in,
    vw_in,
    bw_in,
    head_gain_in,
    ow_in,
    ids_in,
    expert_gain_in,
    router_in,
    gate_in,
    up_in,
    down_in,
    out_ref,
    blocks_ref,
    normed_ref,
    parts_ref,
    passed_ref,
    state_ref,
    residual_ref,
    placed_ref,
    gain_ref,
    qw_ref,
    kw_ref,
    vw_ref,
    bw_ref,
    head_gain_ref,
    ow_ref,
    ids_ref,
    expert_gain_ref,
    router_ref,
    gate_ref,
    up_ref,
    down_ref,
    outgoing_ref,
    arrived_ref,
    result_ref,
    back_ref,
    load_sem,
    own_sem,
    send,
    recv,
    relay_send,
    sum_send,
    sum_recv,
    expert_sem,
    there_send,
    there_recv,
    back_send,
    back_recv,
    keep_sem,
):
    me = lax.axis_index(axis)
    length, width = x_in.shape
    rows = length // n
    chunks = length // rows
    subs = rows // CT
    own = pltpu.make_async_copy(x_in, blocks_ref.at[me], own_sem)
    own.start()
    loads = [
        (gain_in, gain_ref),
        (kw_in, kw_ref),
        (vw_in, vw_ref),
        (qw_in, qw_ref),
        (bw_in, bw_ref),
        (head_gain_in, head_gain_ref),
        (ow_in, ow_ref),
        (ids_in, ids_ref),
        (expert_gain_in, expert_gain_ref),
        (router_in, router_ref),
    ]
    loads = [
        pltpu.make_async_copy(source, target, load_sem.at[i])
        for i, (source, target) in enumerate(loads)
    ]
    for load in loads:
        load.start()
    this = lax.axis_index(owners_axis)
    steps = range(owners - 1, 0, -1)
    peers = {step: lax.rem(this + step, owners) for step in steps}
    barrier = pltpu.get_barrier_semaphore()
    for step in range(1, n):
        pl.semaphore_signal(
            barrier, inc=1, device_id={axis: lax.rem(me + step, n)}, device_id_type=MESH
        )
    for step in steps:
        pl.semaphore_signal(
            barrier, inc=1, device_id={owners_axis: peers[step]}, device_id_type=MESH
        )
    pl.semaphore_wait(barrier, n - 1 + owners - 1)
    own.wait()

    def piece(s, c):
        return blocks_ref.at[s, pl.ds(pl.multiple_of(c * rows, rows), rows)]

    def carry(s, c, send_sem, peer):
        return pltpu.make_async_remote_copy(
            src_ref=piece(s, c),
            dst_ref=piece(s, c),
            send_sem=send_sem,
            recv_sem=recv.at[s, c],
            device_id={axis: peer},
            device_id_type=MESH,
        )

    def own_sends(c, action):
        for step in range(1, n):
            upward, downward = me + step < n, me >= step
            if n == 4 and 1 < step < RELAY_STEPS:
                straight = c < DIRECT
                upward = upward & (straight | (me + step < n - 1))
                downward = downward & (straight | (me > step))

            @pl.when(upward)
            def _():
                action(carry(me, c, send.at[c, step, 0], lax.rem(me + step, n)))

            @pl.when(downward)
            def _():
                action(carry(me, c, send.at[c, step, 1], lax.rem(me + n - step, n)))

    def relays(s, c, action):
        middle = n - 2 if s < n // 2 else 1

        @pl.when((me == middle) & (c >= DIRECT))
        def _():
            action(carry(s, c, relay_send.at[s, c], 0 if s >= n // 2 else n - 1))

    def group(ref, g):
        return ref.at[pl.ds(g * (rows // GROUPS), rows // GROUPS)]

    def passing(way, k, g):
        peer = lax.rem(me + 1, n) if way == 0 else lax.rem(me + n - 1, n)
        return pltpu.make_async_remote_copy(
            src_ref=group(parts_ref.at[k], g),
            dst_ref=group(passed_ref.at[way, k], g),
            send_sem=sum_send.at[k, g],
            recv_sem=sum_recv.at[way, k, g],
            device_id={axis: peer},
            device_id_type=MESH,
        )

    def pass_on(way, k, joins):
        for g in range(GROUPS):
            span = pl.ds(g * (rows // GROUPS), rows // GROUPS)

            @pl.when(joins)
            def _():
                passing(way, k, g).wait_recv()
                parts_ref[k, span] = (
                    parts_ref[k, span].astype(F32) + passed_ref[way, k, span].astype(F32)
                ).astype(BF16)

            passing(way, k, g).start()

    def sum_step(c):
        k_up = c - me
        hops = n - 1 - me
        k_down = c - hops - jnp.minimum(hops, 1)

        @pl.when((k_up > me) & (k_up < n))
        def _():
            pass_on(0, k_up, me > 0)

        @pl.when((k_down >= 0) & (k_down < me))
        def _():
            pass_on(1, k_down, me < n - 1)

    for c in range(min(AHEAD, chunks)):
        own_sends(c, lambda copy: copy.start())
    order = sorted(range(n), key=lambda s: abs(2 * s - (n - 1)))

    for h in range(heads):
        state_ref[h] = jnp.zeros((DK, DK), F32)
    for load in loads:
        load.wait()
    experts = gate_in.shape[0]
    expert_loads = []
    for e in range(experts):
        pairs = ((gate_in, gate_ref), (up_in, up_ref), (down_in, down_ref))
        expert_loads.append(
            [
                pltpu.make_async_copy(source.at[e], target.at[e], expert_sem.at[e, i])
                for i, (source, target) in enumerate(pairs)
            ]
        )
        for load in expert_loads[e]:
            load.start()

    capacity, model_width = outgoing_ref.shape[2:]
    experts_total = router_ref.shape[0]
    slots = experts_total * capacity
    sub, lane = (lax.broadcasted_iota(jnp.int32, (rows, rows), i) for i in (0, 1))
    label = lax.broadcasted_iota(jnp.int32, (rows, experts_total), 1)
    base = ((label % experts) * (owners * capacity) + (label // experts) * capacity).astype(F32)

    def choose(k):
        named = jnp.where(sub == lane, ids_ref[k : k + 1, :].astype(F32), 0.0)
        return jnp.sum(named, -1, keepdims=True) == label.astype(F32)

    picks = sum(choose(k).astype(F32) for k in range(2))
    earlier = dot1((sub > lane).astype(F32), picks)
    slot = lax.broadcasted_iota(jnp.int32, (rows, slots), 1).astype(F32)
    for k in range(2):
        target = jnp.sum(jnp.where(choose(k), earlier + base, 0.0), -1, keepdims=True)
        placed_ref[k] = (slot == target).astype(F32)

    rows_c = NH * CT
    later = lax.broadcasted_iota(jnp.int32, (rows_c, rows_c), 0)
    early = lax.broadcasted_iota(jnp.int32, (rows_c, rows_c), 1)
    later_t, early_t = later % CT, early % CT
    same_token = later_t == early_t
    strict = (early_t < later_t) | (same_token & (early < later))
    eye = (later == early).astype(F32)
    seen = (lax.broadcasted_iota(jnp.int32, (CT, rows_c), 1) % CT) <= lax.broadcasted_iota(
        jnp.int32, (CT, rows_c), 0
    )

    def unit(values):
        return values * lax.rsqrt(jnp.sum(values * values, -1, keepdims=True) + EPSILON)

    def head_of(values, h):
        return values[:, h * DK : (h + 1) * DK]

    def step_chunk(c, _):
        if AHEAD < chunks:

            @pl.when(c + AHEAD < chunks)
            def _():
                own_sends(c + AHEAD, lambda copy: copy.start())

        for s in order:

            @pl.when(me != s)
            def _():
                carry(s, c, send.at[0, 0, 0], lax.rem(me + 1, n)).wait_recv()

            if n == 4 and (RELAY_STEPS > 3 or 0 < s < n - 1):
                relays(s, c, lambda copy: copy.start())
        span = pl.ds(pl.multiple_of(c * rows, rows), rows)
        square = jnp.zeros((rows, 1), F32)
        for s in range(n):
            part = blocks_ref[s, span].astype(F32)
            square = square + jnp.sum(part * part, -1, keepdims=True)
        scale = lax.rsqrt(square / (n * width) + EPSILON)
        for s in range(n):
            cols = pl.ds(s * width, width)
            normed_ref[:, cols] = (
                blocks_ref[s, span].astype(F32) * scale * gain_ref[:, cols]
            ).astype(BF16)

        def project(weight):
            return jnp.dot(normed_ref[...], weight, preferred_element_type=F32)

        key_parts = [project(kw_ref[m]) for m in range(NH)]
        beta = 2.0 / (
            1.0
            + jnp.exp(
                -lax.dot_general(normed_ref[...], bw_ref[...], NT, preferred_element_type=F32)
            )
        )

        def rows_of(member_parts, j):
            return jnp.concatenate(
                [part[j * CT : (j + 1) * CT] for part in member_parts], 0
            )

        cases = [(h, j) for h in range(heads) for j in range(subs)]
        units = [[unit(head_of(part, h)) for part in key_parts] for h in range(heads)]
        all_keys, all_scaled, betas, parts = [], [], [], []
        for h, j in cases:
            keys = rows_of(units[h], j)
            betas.append(
                rows_of([beta[:, h * NH + m : h * NH + m + 1] for m in range(NH)], j)
            )
            scaled = keys * betas[-1]
            all_scaled.append(scaled)
            all_keys.append(halves(keys))
            similar = dot3(halves(scaled), all_keys[-1], NT)
            parts.append(jnp.where(strict, similar, 0.0))
        inverses = []
        for part in parts:
            inner = jnp.where(same_token, part, 0.0)
            inverses.append(eye - inner + dot1(inner, inner))
        side = [lambda m=m: project(vw_ref[m]) for m in range(NH)]
        side.append(lambda: project(qw_ref[...]))
        side_parts = []
        size = 1
        while size < CT:
            joined = (later_t // (2 * size) == early_t // (2 * size)) & (
                later_t // size != early_t // size
            )
            steps = [
                dot1(jnp.where(joined, part, 0.0), inverse)
                for part, inverse in zip(parts, inverses)
            ]
            if side:
                side_parts.append(side.pop(0)())
            inverses = [
                inverse - dot1(inverse, step) for inverse, step in zip(inverses, steps)
            ]
            size *= 2
        while side:
            side_parts.append(side.pop(0)())
        value_parts, query_part = side_parts[:NH], side_parts[NH]
        queries = [
            halves(unit(head_of(query_part, h))[j * CT : (j + 1) * CT] * DK ** (-0.5))
            for h, j in cases
        ]
        rights = [
            jnp.concatenate(
                [scaled, rows_of([head_of(part, h) for part in value_parts], j) * betas_now], 1
            )
            for (h, j), scaled, betas_now in zip(cases, all_scaled, betas)
        ]
        guesses = [dot1(inverse, right) for inverse, right in zip(inverses, rights)]
        attends = [
            halves(jnp.where(seen, dot3(query, keys, NT), 0.0))
            for query, keys in zip(queries, all_keys)
        ]
        rests = [
            right - guess - dot3(halves(part), halves(guess))
            for right, guess, part in zip(rights, guesses, parts)
        ]
        all_solved = [
            guess + dot1(inverse, rest)
            for guess, inverse, rest in zip(guesses, inverses, rests)
        ]
        befores = [state_ref[h] for h in range(heads)]
        mixes = [[] for _ in range(heads)]
        for j in range(subs):
            for h in range(heads):
                i = h * subs + j
                state = halves(befores[h])
                solved = all_solved[i]
                corrected = solved[:, DK:] - dot3(halves(solved[:, :DK]), state)
                split = halves(corrected)
                mixed = dot3(queries[i], state) + dot3(attends[i], split)
                befores[h] = befores[h] + dot3(all_keys[i], split, TN)
                mixes[h].append(root_norm(mixed, head_gain_ref[...]).astype(BF16))
        for h in range(heads):
            state_ref[h] = befores[h]
        mixes = [jnp.concatenate(mix, 0) for mix in mixes]
        parts_ref[c] = jnp.dot(
            jnp.concatenate(mixes, 1), ow_ref[...], preferred_element_type=F32
        ).astype(BF16)
        sum_step(c)
        return 0

    lax.fori_loop(0, chunks, step_chunk, 0)
    for c in range(chunks, 2 * n):
        sum_step(c)
    mine = pl.ds(pl.multiple_of(me * rows, rows), rows)
    for s in range(n):
        cols = pl.ds(s * width, width)
        residual_ref[:, cols] = blocks_ref[s, mine].astype(F32) + parts_ref[me, :, cols].astype(F32)
    for way, comes in ((0, me > 0), (1, me < n - 1)):
        for g in range(GROUPS):
            span = pl.ds(g * (rows // GROUPS), rows // GROUPS)

            @pl.when(comes)
            def _():
                passing(way, me, g).wait_recv()
                residual_ref[span] += passed_ref[way, me, span].astype(F32)

    residual = residual_ref[...]
    routed = root_norm(residual, expert_gain_ref[...])
    spread = (placed_ref[0] + placed_ref[1]).astype(BF16)
    expert_rows = routed.astype(BF16)
    copies, keeps = [], []

    def across(source, target, sends, receives, e, step):
        return pltpu.make_async_remote_copy(
            src_ref=source.at[e, peers[step]],
            dst_ref=target.at[e, this],
            send_sem=sends.at[e, step],
            recv_sem=receives.at[e, step],
            device_id={owners_axis: peers[step]},
            device_id_type=MESH,
        )

    def keep(source, target, i, e):
        keeps.append(
            pltpu.make_async_copy(source.at[e, this], target.at[e, this], keep_sem.at[i, e])
        )
        keeps[-1].start()
        return keeps[-1]

    kept = []
    for e in range(experts):
        here = spread[:, e * owners * capacity : (e + 1) * owners * capacity]
        outgoing = lax.dot_general(
            here, expert_rows, TN, preferred_element_type=F32
        ).astype(BF16)
        for s in range(owners):
            outgoing_ref[e, s] = outgoing[s * capacity : (s + 1) * capacity]
        copies.append([])
        for step in steps:
            copies[e].append(
                across(outgoing_ref, arrived_ref, there_send, there_recv, e, step)
            )
            copies[e][-1].start()
        kept.append(keep(outgoing_ref, arrived_ref, 0, e))
    logits = lax.dot_general(
        routed, router_ref[...], NT, precision=TOP_PRECISION, preferred_element_type=F32
    )
    chosen = [jnp.sum(jnp.where(choose(k), logits, 0.0), -1, keepdims=True) for k in range(2)]
    leading = 1.0 / (1.0 + jnp.exp(chosen[1] - chosen[0]))
    weights = placed_ref[0] * leading + placed_ref[1] * (1.0 - leading)
    stacked = jnp.concatenate(halves(weights), 0)
    returns = []
    for e in range(experts):
        for copy in copies[e]:
            copy.wait_recv()
        kept[e].wait()
        arrived = jnp.concatenate([arrived_ref[e, s] for s in range(owners)], 0)
        expert_loads[e][0].wait()
        gated = jnp.dot(arrived, gate_ref[e], preferred_element_type=F32)
        expert_loads[e][1].wait()
        lifted = jnp.dot(arrived, up_ref[e], preferred_element_type=F32)
        hidden = (gated / (1.0 + jnp.exp(-gated)) * lifted).astype(BF16)
        expert_loads[e][2].wait()
        made = jnp.dot(hidden, down_ref[e], preferred_element_type=F32).astype(BF16)
        for s in range(owners):
            result_ref[e, s] = made[s * capacity : (s + 1) * capacity]
        returns.append([])
        for step in steps:
            returns[e].append(across(result_ref, back_ref, back_send, back_recv, e, step))
            returns[e][-1].start()
        kept.append(keep(result_ref, back_ref, 1, e))
    blended = residual_ref[...]
    for e in range(experts):
        for copy in returns[e]:
            copy.wait_recv()
        kept[experts + e].wait()
        back = jnp.concatenate([back_ref[e, s] for s in range(owners)], 0)
        share = stacked[:, e * owners * capacity : (e + 1) * owners * capacity]
        both = jnp.dot(share, back, preferred_element_type=F32)
        blended = blended + (both[:rows] + both[rows:])
    out_ref[...] = blended.astype(BF16)
    for copy in sum(copies + returns, []):
        copy.wait_send()

    for c in range(n):

        @pl.when(me != c)
        def _():
            for g in range(GROUPS):
                passing(0, c, g).wait_send()

    for c in range(chunks):
        own_sends(c, lambda copy: copy.wait_send())
        if n == 4:
            for s in range(n) if RELAY_STEPS > 3 else range(1, n - 1):
                relays(s, c, lambda copy: copy.wait_send())


def layer(axis, n, owners_axis, owners, x, *arrays):
    length, width = x.shape
    qw, kw, vw, bw, head_gain, ow, expert_gain, router, ids, gate, up, down = arrays[1:]
    heads = qw.shape[1] // DK
    model_width = n * width
    chunks, rows = n, length // n
    experts = gate.shape[0]
    capacity = 4 * rows // router.shape[1]
    gain, head_gain, expert_gain = (
        values.reshape(1, -1) for values in (arrays[0], head_gain, expert_gain)
    )
    small = (gain, qw, kw, vw, bw.T, head_gain, ow, ids.T, expert_gain, router.T)
    slotted = pltpu.VMEM((experts, owners, capacity, model_width), BF16)
    peer_sems = pltpu.SemaphoreType.DMA((experts, owners))
    return pl.pallas_call(
        functools.partial(layer_kernel, axis, n, heads, owners_axis, owners),
        out_shape=jax.ShapeDtypeStruct((rows, model_width), BF16),
        in_specs=[ANY] * 14,
        out_specs=VMEM,
        scratch_shapes=[
            pltpu.VMEM((n, length, width), BF16),
            pltpu.VMEM((rows, model_width), BF16),
            pltpu.VMEM((chunks, rows, model_width), BF16),
            pltpu.VMEM((2, chunks, rows, model_width), BF16),
            pltpu.VMEM((heads, DK, DK), F32),
            pltpu.VMEM((rows, model_width), F32),
            pltpu.VMEM((2, rows, router.shape[1] * capacity), F32),
        ]
        + [pltpu.VMEM(array.shape, array.dtype) for array in small + (gate, up, down)]
        + [slotted] * 4
        + [
            pltpu.SemaphoreType.DMA((len(small),)),
            pltpu.SemaphoreType.DMA,
            pltpu.SemaphoreType.DMA((chunks, n, 2)),
            pltpu.SemaphoreType.DMA((n, chunks)),
            pltpu.SemaphoreType.DMA((n, chunks)),
            pltpu.SemaphoreType.DMA((chunks, GROUPS)),
            pltpu.SemaphoreType.DMA((2, chunks, GROUPS)),
            pltpu.SemaphoreType.DMA((experts, 3)),
            peer_sems,
            peer_sems,
            peer_sems,
            peer_sems,
            pltpu.SemaphoreType.DMA((2, experts)),
        ],
        compiler_params=pltpu.CompilerParams(
            collective_id=0, has_side_effects=True, vmem_limit_bytes=63 << 20
        ),
        cost_estimate=pl.CostEstimate(
            flops=20 << 30, bytes_accessed=50 << 20, transcendentals=0
        ),
        name="layer",
    )(x, *small, gate, up, down)


def shards(heads_axis, owners, *arrays):
    return layer("head", heads_axis, "dp", owners, *arrays)


def solution(mesh):
    return jax.shard_map(
        functools.partial(shards, mesh.shape["head"], mesh.shape["dp"]),
        mesh=mesh,
        in_specs=(
            P("dp", "head"),
            P(),
            P(None, "head"),
            P(None, None, "head"),
            P(None, None, "head"),
            P(None, "head"),
            P(),
            P("head", None),
            P(),
            P(),
            P(("dp", "head"), None),
            P("dp", None, None),
            P("dp", None, None),
            P("dp", None, None),
        ),
        out_specs=P(("dp", "head"), None),
        check_vma=False,
    )
```

```python
import functools

import jax
import jax.numpy as jnp
from jax import lax
from jax.experimental import pallas as pl
from jax.experimental.pallas import tpu as pltpu
from jax.sharding import PartitionSpec as P

DK = 128
NH = 3
CT = 32
GROUPS = 8
AHEAD = 3


EPSILON = 1e-06
TOP_PRECISION = lax.Precision.HIGHEST
MESH = pl.DeviceIdType.MESH
VMEM = pl.BlockSpec(memory_space=pltpu.VMEM)
ANY = pl.BlockSpec(memory_space=pl.ANY)
HBM = pl.BlockSpec(memory_space=pltpu.HBM)
F32 = jnp.float32
BF16 = jnp.bfloat16


def root_norm(values, gain):
    return values * lax.rsqrt(jnp.mean(values * values, -1, keepdims=True) + EPSILON) * gain


NN = (((1,), (0,)), ((), ()))
NT = (((1,), (1,)), ((), ()))
TN = (((0,), (0,)), ((), ()))


def dot1(a, b, dims=NN):
    return lax.dot_general(a.astype(BF16), b.astype(BF16), dims, preferred_element_type=F32)


def halves(a):
    high = a.astype(BF16)
    return high, (a - high.astype(F32)).astype(BF16)


def dot3(a, b, dims=NN):
    ah, al = a
    bh, bl = b
    product = functools.partial(
        lax.dot_general, dimension_numbers=dims, preferred_element_type=F32
    )
    return product(ah, bh) + (product(ah, bl) + product(al, bh))


def layer_kernel(
    axis,
    n,
    heads,
    owners_axis,
    owners,
    x_in,
    gain_in,
    qw_in,
    kw_in,
    vw_in,
    bw_in,
    head_gain_in,
    ow_in,
    ids_in,
    expert_gain_in,
    router_in,
    gate_in,
    up_in,
    down_in,
    out_ref,
    blocks_ref,
    normed_ref,
    parts_ref,
    passed_ref,
    straight_ref,
    state_ref,
    residual_ref,
    placed_ref,
    gain_ref,
    qw_ref,
    kw_ref,
    vw_ref,
    bw_ref,
    head_gain_ref,
    ow_ref,
    ids_ref,
    expert_gain_ref,
    router_ref,
    gate_ref,
    up_ref,
    down_ref,
    outgoing_ref,
    arrived_ref,
    result_ref,
    back_ref,
    load_sem,
    own_sem,
    send,
    recv,
    relay_send,
    sum_send,
    sum_recv,
    straight_recv,
    expert_sem,
    there_send,
    there_recv,
    back_send,
    back_recv,
    keep_sem,
):
    me = lax.axis_index(axis)
    length, width = x_in.shape
    rows = length // n
    chunks = length // rows
    subs = rows // CT
    own = pltpu.make_async_copy(x_in, blocks_ref.at[me], own_sem)
    own.start()
    loads = [
        (gain_in, gain_ref),
        (kw_in, kw_ref),
        (vw_in, vw_ref),
        (qw_in, qw_ref),
        (bw_in, bw_ref),
        (head_gain_in, head_gain_ref),
        (ow_in, ow_ref),
        (ids_in, ids_ref),
        (expert_gain_in, expert_gain_ref),
        (router_in, router_ref),
    ]
    loads = [
        pltpu.make_async_copy(source, target, load_sem.at[i])
        for i, (source, target) in enumerate(loads)
    ]
    for load in loads:
        load.start()
    this = lax.axis_index(owners_axis)
    steps = range(owners - 1, 0, -1)
    peers = {step: lax.rem(this + step, owners) for step in steps}
    barrier = pltpu.get_barrier_semaphore()
    for step in range(1, n):
        pl.semaphore_signal(
            barrier, inc=1, device_id={axis: lax.rem(me + step, n)}, device_id_type=MESH
        )
    for step in steps:
        pl.semaphore_signal(
            barrier, inc=1, device_id={owners_axis: peers[step]}, device_id_type=MESH
        )
    pl.semaphore_wait(barrier, n - 1 + owners - 1)
    own.wait()

    def piece(s, c):
        return blocks_ref.at[s, pl.ds(pl.multiple_of(c * rows, rows), rows)]

    def carry(s, c, send_sem, peer):
        return pltpu.make_async_remote_copy(
            src_ref=piece(s, c),
            dst_ref=piece(s, c),
            send_sem=send_sem,
            recv_sem=recv.at[s, c],
            device_id={axis: peer},
            device_id_type=MESH,
        )

    def own_sends(c, action):
        for step in range(1, n):
            upward, downward = me + step < n, me >= step
            if n == 4 and step > 1:
                upward, downward = me + step < n - 1, me > step

            @pl.when(upward)
            def _():
                action(carry(me, c, send.at[c, step, 0], lax.rem(me + step, n)))

            @pl.when(downward)
            def _():
                action(carry(me, c, send.at[c, step, 1], lax.rem(me + n - step, n)))

    def middle_of(s):
        return (n - 2 if s < n // 2 else 1) if n == 4 else -1

    def relay(s, c):
        return carry(s, c, relay_send.at[s, c], 0 if s >= n // 2 else n - 1)

    def hand_on(s, c, due):
        @pl.when((me == middle_of(s)) & due)
        def _():
            relay(s, c).wait_recv()
            relay(s, c).start()

    def group(ref, g):
        return ref.at[pl.ds(g * (rows // GROUPS), rows // GROUPS)]

    def passing(way, k, g):
        peer = lax.rem(me + 1, n) if way == 0 else lax.rem(me + n - 1, n)
        return pltpu.make_async_remote_copy(
            src_ref=group(parts_ref.at[k], g),
            dst_ref=group(passed_ref.at[way, k], g),
            send_sem=sum_send.at[k, g],
            recv_sem=sum_recv.at[way, k, g],
            device_id={axis: peer},
            device_id_type=MESH,
        )

    def pass_on(way, k, joins):
        for g in range(GROUPS):
            span = pl.ds(g * (rows // GROUPS), rows // GROUPS)

            @pl.when(joins)
            def _():
                passing(way, k, g).wait_recv()
                parts_ref[k, span] = (
                    parts_ref[k, span].astype(F32) + passed_ref[way, k, span].astype(F32)
                ).astype(BF16)

            passing(way, k, g).start()

    def straight(g):
        return pltpu.make_async_remote_copy(
            src_ref=group(parts_ref.at[n - 1], g),
            dst_ref=group(straight_ref, g),
            send_sem=sum_send.at[n - 1, g],
            recv_sem=straight_recv.at[g],
            device_id={axis: n - 1},
            device_id_type=MESH,
        )

    def sum_step(c):
        k_up = c - me - jnp.minimum(me, 1)
        hops = n - 1 - me
        k_down = c - hops - jnp.minimum(hops, 1)

        @pl.when((me == 0) & (c == n - 1))
        def _():
            for g in range(GROUPS):
                straight(g).start()

        @pl.when((me > 0) & (me < n - 1) & (c == n - 2 + me))
        def _():
            pass_on(0, n - 1, me > 1)

        @pl.when((k_up > me) & (k_up < n - 1))
        def _():
            pass_on(0, k_up, me > 0)

        @pl.when((k_down >= 0) & (k_down < me))
        def _():
            pass_on(1, k_down, me < n - 1)

    for c in range(min(AHEAD, chunks)):
        own_sends(c, lambda copy: copy.start())
    order = sorted(range(n), key=lambda s: abs(2 * s - (n - 1)))

    for h in range(heads):
        state_ref[h] = jnp.zeros((DK, DK), F32)
    for load in loads:
        load.wait()
    experts = gate_in.shape[0]
    expert_loads = []
    for e in range(experts):
        pairs = ((gate_in, gate_ref), (up_in, up_ref), (down_in, down_ref))
        expert_loads.append(
            [
                pltpu.make_async_copy(source.at[e], target.at[e], expert_sem.at[e, i])
                for i, (source, target) in enumerate(pairs)
            ]
        )
        for load in expert_loads[e]:
            load.start()

    capacity, model_width = outgoing_ref.shape[2:]
    experts_total = router_ref.shape[0]
    slots = experts_total * capacity
    sub, lane = (lax.broadcasted_iota(jnp.int32, (rows, rows), i) for i in (0, 1))
    label = lax.broadcasted_iota(jnp.int32, (rows, experts_total), 1)
    base = ((label % experts) * (owners * capacity) + (label // experts) * capacity).astype(F32)

    def choose(k):
        named = jnp.where(sub == lane, ids_ref[k : k + 1, :].astype(F32), 0.0)
        return jnp.sum(named, -1, keepdims=True) == label.astype(F32)

    picks = sum(choose(k).astype(F32) for k in range(2))
    earlier = dot1((sub > lane).astype(F32), picks)
    slot = lax.broadcasted_iota(jnp.int32, (rows, slots), 1).astype(F32)
    for k in range(2):
        target = jnp.sum(jnp.where(choose(k), earlier + base, 0.0), -1, keepdims=True)
        placed_ref[k] = (slot == target).astype(F32)

    rows_c = NH * CT
    later = lax.broadcasted_iota(jnp.int32, (rows_c, rows_c), 0)
    early = lax.broadcasted_iota(jnp.int32, (rows_c, rows_c), 1)
    later_t, early_t = later % CT, early % CT
    same_token = later_t == early_t
    strict = (early_t < later_t) | (same_token & (early < later))
    eye = (later == early).astype(F32)
    seen = (lax.broadcasted_iota(jnp.int32, (CT, rows_c), 1) % CT) <= lax.broadcasted_iota(
        jnp.int32, (CT, rows_c), 0
    )

    def unit(values):
        return values * lax.rsqrt(jnp.sum(values * values, -1, keepdims=True) + EPSILON)

    def head_of(values, h):
        return values[:, h * DK : (h + 1) * DK]

    def step_chunk(c, _):
        if AHEAD < chunks:

            @pl.when(c + AHEAD < chunks)
            def _():
                own_sends(c + AHEAD, lambda copy: copy.start())

        if n == 4:
            for s in order:
                hand_on(s, c, c == 0)
            for s in order:
                hand_on(s, c + 1, c + 1 < chunks)
        for s in order:

            @pl.when((me != s) & (me != middle_of(s)))
            def _():
                carry(s, c, send.at[0, 0, 0], lax.rem(me + 1, n)).wait_recv()

        span = pl.ds(pl.multiple_of(c * rows, rows), rows)
        square = jnp.zeros((rows, 1), F32)
        for s in range(n):
            part = blocks_ref[s, span].astype(F32)
            square = square + jnp.sum(part * part, -1, keepdims=True)
        scale = lax.rsqrt(square / (n * width) + EPSILON)
        for s in range(n):
            cols = pl.ds(s * width, width)
            normed_ref[:, cols] = (
                blocks_ref[s, span].astype(F32) * scale * gain_ref[:, cols]
            ).astype(BF16)

        def project(weight):
            return jnp.dot(normed_ref[...], weight, preferred_element_type=F32)

        key_parts = [project(kw_ref[m]) for m in range(NH)]
        beta = 2.0 / (
            1.0
            + jnp.exp(
                -lax.dot_general(normed_ref[...], bw_ref[...], NT, preferred_element_type=F32)
            )
        )

        def rows_of(member_parts, j):
            return jnp.concatenate(
                [part[j * CT : (j + 1) * CT] for part in member_parts], 0
            )

        cases = [(h, j) for h in range(heads) for j in range(subs)]
        units = [[unit(head_of(part, h)) for part in key_parts] for h in range(heads)]
        all_keys, all_scaled, betas, parts = [], [], [], []
        for h, j in cases:
            keys = rows_of(units[h], j)
            betas.append(
                rows_of([beta[:, h * NH + m : h * NH + m + 1] for m in range(NH)], j)
            )
            scaled = keys * betas[-1]
            all_scaled.append(scaled)
            all_keys.append(halves(keys))
            similar = dot3(halves(scaled), all_keys[-1], NT)
            parts.append(jnp.where(strict, similar, 0.0))
        inverses = []
        for part in parts:
            inner = jnp.where(same_token, part, 0.0)
            inverses.append(eye - inner + dot1(inner, inner))
        side = [lambda m=m: project(vw_ref[m]) for m in range(NH)]
        side.append(lambda: project(qw_ref[...]))
        side_parts = []
        size = 1
        while size < CT:
            joined = (later_t // (2 * size) == early_t // (2 * size)) & (
                later_t // size != early_t // size
            )
            steps = [
                dot1(jnp.where(joined, part, 0.0), inverse)
                for part, inverse in zip(parts, inverses)
            ]
            if side:
                side_parts.append(side.pop(0)())
            inverses = [
                inverse - dot1(inverse, step) for inverse, step in zip(inverses, steps)
            ]
            size *= 2
        while side:
            side_parts.append(side.pop(0)())
        value_parts, query_part = side_parts[:NH], side_parts[NH]
        queries = [
            halves(unit(head_of(query_part, h))[j * CT : (j + 1) * CT] * DK ** (-0.5))
            for h, j in cases
        ]
        rights = [
            jnp.concatenate(
                [scaled, rows_of([head_of(part, h) for part in value_parts], j) * betas_now], 1
            )
            for (h, j), scaled, betas_now in zip(cases, all_scaled, betas)
        ]
        guesses = [dot1(inverse, right) for inverse, right in zip(inverses, rights)]
        attends = [
            halves(jnp.where(seen, dot3(query, keys, NT), 0.0))
            for query, keys in zip(queries, all_keys)
        ]
        rests = [
            right - guess - dot3(halves(part), halves(guess))
            for right, guess, part in zip(rights, guesses, parts)
        ]
        all_solved = [
            guess + dot1(inverse, rest)
            for guess, inverse, rest in zip(guesses, inverses, rests)
        ]
        befores = [state_ref[h] for h in range(heads)]
        mixes = [[] for _ in range(heads)]
        for j in range(subs):
            for h in range(heads):
                i = h * subs + j
                state = halves(befores[h])
                solved = all_solved[i]
                corrected = solved[:, DK:] - dot3(halves(solved[:, :DK]), state)
                split = halves(corrected)
                mixed = dot3(queries[i], state) + dot3(attends[i], split)
                befores[h] = befores[h] + dot3(all_keys[i], split, TN)
                mixes[h].append(root_norm(mixed, head_gain_ref[...]).astype(BF16))
        for h in range(heads):
            state_ref[h] = befores[h]
        mixes = [jnp.concatenate(mix, 0) for mix in mixes]
        parts_ref[c] = jnp.dot(
            jnp.concatenate(mixes, 1), ow_ref[...], preferred_element_type=F32
        ).astype(BF16)
        sum_step(c)
        return 0

    lax.fori_loop(0, chunks, step_chunk, 0)
    for c in range(chunks, 2 * n):
        sum_step(c)
    mine = pl.ds(pl.multiple_of(me * rows, rows), rows)
    for s in range(n):
        cols = pl.ds(s * width, width)
        residual_ref[:, cols] = blocks_ref[s, mine].astype(F32) + parts_ref[me, :, cols].astype(F32)
    for way, comes in ((0, me > 0), (1, me < n - 1)):
        for g in range(GROUPS):
            span = pl.ds(g * (rows // GROUPS), rows // GROUPS)

            @pl.when(comes)
            def _():
                passing(way, me, g).wait_recv()
                residual_ref[span] += passed_ref[way, me, span].astype(F32)

    for g in range(GROUPS):
        span = pl.ds(g * (rows // GROUPS), rows // GROUPS)

        @pl.when(me == n - 1)
        def _():
            straight(g).wait_recv()
            residual_ref[span] += straight_ref[span].astype(F32)

    residual = residual_ref[...]
    routed = root_norm(residual, expert_gain_ref[...])
    spread = (placed_ref[0] + placed_ref[1]).astype(BF16)
    expert_rows = routed.astype(BF16)
    copies, keeps = [], []

    def across(source, target, sends, receives, e, step):
        return pltpu.make_async_remote_copy(
            src_ref=source.at[e, peers[step]],
            dst_ref=target.at[e, this],
            send_sem=sends.at[e, step],
            recv_sem=receives.at[e, step],
            device_id={owners_axis: peers[step]},
            device_id_type=MESH,
        )

    def keep(source, target, i, e):
        keeps.append(
            pltpu.make_async_copy(source.at[e, this], target.at[e, this], keep_sem.at[i, e])
        )
        keeps[-1].start()
        return keeps[-1]

    kept = []
    for e in range(experts):
        here = spread[:, e * owners * capacity : (e + 1) * owners * capacity]
        outgoing = lax.dot_general(
            here, expert_rows, TN, preferred_element_type=F32
        ).astype(BF16)
        for s in range(owners):
            outgoing_ref[e, s] = outgoing[s * capacity : (s + 1) * capacity]
        copies.append([])
        for step in steps:
            copies[e].append(
                across(outgoing_ref, arrived_ref, there_send, there_recv, e, step)
            )
            copies[e][-1].start()
        kept.append(keep(outgoing_ref, arrived_ref, 0, e))
    logits = lax.dot_general(
        routed, router_ref[...], NT, precision=TOP_PRECISION, preferred_element_type=F32
    )
    chosen = [jnp.sum(jnp.where(choose(k), logits, 0.0), -1, keepdims=True) for k in range(2)]
    leading = 1.0 / (1.0 + jnp.exp(chosen[1] - chosen[0]))
    weights = placed_ref[0] * leading + placed_ref[1] * (1.0 - leading)
    stacked = jnp.concatenate(halves(weights), 0)
    returns = []
    for e in range(experts):
        for copy in copies[e]:
            copy.wait_recv()
        kept[e].wait()
        arrived = jnp.concatenate([arrived_ref[e, s] for s in range(owners)], 0)
        expert_loads[e][0].wait()
        gated = jnp.dot(arrived, gate_ref[e], preferred_element_type=F32)
        expert_loads[e][1].wait()
        lifted = jnp.dot(arrived, up_ref[e], preferred_element_type=F32)
        hidden = (gated / (1.0 + jnp.exp(-gated)) * lifted).astype(BF16)
        expert_loads[e][2].wait()
        made = jnp.dot(hidden, down_ref[e], preferred_element_type=F32).astype(BF16)
        for s in range(owners):
            result_ref[e, s] = made[s * capacity : (s + 1) * capacity]
        returns.append([])
        for step in steps:
            returns[e].append(across(result_ref, back_ref, back_send, back_recv, e, step))
            returns[e][-1].start()
        kept.append(keep(result_ref, back_ref, 1, e))
    blended = residual_ref[...]
    for e in range(experts):
        for copy in returns[e]:
            copy.wait_recv()
        kept[experts + e].wait()
        back = jnp.concatenate([back_ref[e, s] for s in range(owners)], 0)
        share = stacked[:, e * owners * capacity : (e + 1) * owners * capacity]
        both = jnp.dot(share, back, preferred_element_type=F32)
        blended = blended + (both[:rows] + both[rows:])
    out_ref[...] = blended.astype(BF16)
    for copy in sum(copies + returns, []):
        copy.wait_send()

    for c in range(n):

        @pl.when(me != c)
        def _():
            for g in range(GROUPS):
                passing(0, c, g).wait_send()

    for c in range(chunks):
        own_sends(c, lambda copy: copy.wait_send())
        if n == 4:
            for s in range(n):

                @pl.when(me == middle_of(s))
                def _():
                    relay(s, c).wait_send()


def layer(axis, n, owners_axis, owners, x, *arrays):
    length, width = x.shape
    qw, kw, vw, bw, head_gain, ow, expert_gain, router, ids, gate, up, down = arrays[1:]
    heads = qw.shape[1] // DK
    model_width = n * width
    chunks, rows = n, length // n
    experts = gate.shape[0]
    capacity = 4 * rows // router.shape[1]
    gain, head_gain, expert_gain = (
        values.reshape(1, -1) for values in (arrays[0], head_gain, expert_gain)
    )
    small = (gain, qw, kw, vw, bw.T, head_gain, ow, ids.T, expert_gain, router.T)
    slotted = pltpu.VMEM((experts, owners, capacity, model_width), BF16)
    peer_sems = pltpu.SemaphoreType.DMA((experts, owners))
    return pl.pallas_call(
        functools.partial(layer_kernel, axis, n, heads, owners_axis, owners),
        out_shape=jax.ShapeDtypeStruct((rows, model_width), BF16),
        in_specs=[ANY] * 14,
        out_specs=VMEM,
        scratch_shapes=[
            pltpu.VMEM((n, length, width), BF16),
            pltpu.VMEM((rows, model_width), BF16),
            pltpu.VMEM((chunks, rows, model_width), BF16),
            pltpu.VMEM((2, chunks, rows, model_width), BF16),
            pltpu.VMEM((rows, model_width), BF16),
            pltpu.VMEM((heads, DK, DK), F32),
            pltpu.VMEM((rows, model_width), F32),
            pltpu.VMEM((2, rows, router.shape[1] * capacity), F32),
        ]
        + [pltpu.VMEM(array.shape, array.dtype) for array in small + (gate, up, down)]
        + [slotted] * 4
        + [
            pltpu.SemaphoreType.DMA((len(small),)),
            pltpu.SemaphoreType.DMA,
            pltpu.SemaphoreType.DMA((chunks, n, 2)),
            pltpu.SemaphoreType.DMA((n, chunks)),
            pltpu.SemaphoreType.DMA((n, chunks)),
            pltpu.SemaphoreType.DMA((chunks, GROUPS)),
            pltpu.SemaphoreType.DMA((2, chunks, GROUPS)),
            pltpu.SemaphoreType.DMA((GROUPS,)),
            pltpu.SemaphoreType.DMA((experts, 3)),
            peer_sems,
            peer_sems,
            peer_sems,
            peer_sems,
            pltpu.SemaphoreType.DMA((2, experts)),
        ],
        compiler_params=pltpu.CompilerParams(
            collective_id=0, has_side_effects=True, vmem_limit_bytes=63 << 20
        ),
        cost_estimate=pl.CostEstimate(
            flops=20 << 30, bytes_accessed=50 << 20, transcendentals=0
        ),
        name="layer",
    )(x, *small, gate, up, down)


def shards(heads_axis, owners, *arrays):
    return layer("head", heads_axis, "dp", owners, *arrays)


def solution(mesh):
    return jax.shard_map(
        functools.partial(shards, mesh.shape["head"], mesh.shape["dp"]),
        mesh=mesh,
        in_specs=(
            P("dp", "head"),
            P(),
            P(None, "head"),
            P(None, None, "head"),
            P(None, None, "head"),
            P(None, "head"),
            P(),
            P("head", None),
            P(),
            P(),
            P(("dp", "head"), None),
            P("dp", None, None),
            P("dp", None, None),
            P("dp", None, None),
        ),
        out_specs=P(("dp", "head"), None),
        check_vma=False,
    )
```

```python
import functools

import jax
import jax.numpy as jnp
from jax import lax
from jax.experimental import pallas as pl
from jax.experimental.pallas import tpu as pltpu
from jax.sharding import PartitionSpec as P

DK = 128
NH = 3
CT = 32
GROUPS = 8
AHEAD = 3


EPSILON = 1e-06
TOP_PRECISION = lax.Precision.HIGHEST
MESH = pl.DeviceIdType.MESH
VMEM = pl.BlockSpec(memory_space=pltpu.VMEM)
ANY = pl.BlockSpec(memory_space=pl.ANY)
HBM = pl.BlockSpec(memory_space=pltpu.HBM)
F32 = jnp.float32
BF16 = jnp.bfloat16


def root_norm(values, gain):
    return values * lax.rsqrt(jnp.mean(values * values, -1, keepdims=True) + EPSILON) * gain


NN = (((1,), (0,)), ((), ()))
NT = (((1,), (1,)), ((), ()))
TN = (((0,), (0,)), ((), ()))


def dot1(a, b, dims=NN):
    return lax.dot_general(a.astype(BF16), b.astype(BF16), dims, preferred_element_type=F32)


def halves(a):
    high = a.astype(BF16)
    return high, (a - high.astype(F32)).astype(BF16)


def dot3(a, b, dims=NN):
    ah, al = a
    bh, bl = b
    product = functools.partial(
        lax.dot_general, dimension_numbers=dims, preferred_element_type=F32
    )
    return product(ah, bh) + (product(ah, bl) + product(al, bh))


def layer_kernel(
    axis,
    n,
    heads,
    owners_axis,
    owners,
    x_in,
    gain_in,
    qw_in,
    kw_in,
    vw_in,
    bw_in,
    head_gain_in,
    ow_in,
    ids_in,
    expert_gain_in,
    router_in,
    gate_in,
    up_in,
    down_in,
    out_ref,
    blocks_ref,
    normed_ref,
    parts_ref,
    passed_ref,
    state_ref,
    residual_ref,
    placed_ref,
    gain_ref,
    qw_ref,
    kw_ref,
    vw_ref,
    bw_ref,
    head_gain_ref,
    ow_ref,
    ids_ref,
    expert_gain_ref,
    router_ref,
    gate_ref,
    up_ref,
    down_ref,
    outgoing_ref,
    arrived_ref,
    result_ref,
    back_ref,
    load_sem,
    own_sem,
    send,
    recv,
    relay_send,
    sum_send,
    sum_recv,
    expert_sem,
    there_send,
    there_recv,
    back_send,
    back_recv,
    keep_sem,
):
    me = lax.axis_index(axis)
    length, width = x_in.shape
    rows = length // n
    chunks = length // rows
    subs = rows // CT
    own = pltpu.make_async_copy(x_in, blocks_ref.at[me], own_sem)
    own.start()
    loads = [
        (gain_in, gain_ref),
        (kw_in, kw_ref),
        (vw_in, vw_ref),
        (qw_in, qw_ref),
        (bw_in, bw_ref),
        (head_gain_in, head_gain_ref),
        (ow_in, ow_ref),
        (ids_in, ids_ref),
        (expert_gain_in, expert_gain_ref),
        (router_in, router_ref),
    ]
    loads = [
        pltpu.make_async_copy(source, target, load_sem.at[i])
        for i, (source, target) in enumerate(loads)
    ]
    for load in loads:
        load.start()
    this = lax.axis_index(owners_axis)
    steps = range(owners - 1, 0, -1)
    peers = {step: lax.rem(this + step, owners) for step in steps}
    barrier = pltpu.get_barrier_semaphore()
    for step in range(1, n):
        pl.semaphore_signal(
            barrier, inc=1, device_id={axis: lax.rem(me + step, n)}, device_id_type=MESH
        )
    for step in steps:
        pl.semaphore_signal(
            barrier, inc=1, device_id={owners_axis: peers[step]}, device_id_type=MESH
        )
    pl.semaphore_wait(barrier, n - 1 + owners - 1)
    own.wait()

    def piece(s, c):
        return blocks_ref.at[s, pl.ds(pl.multiple_of(c * rows, rows), rows)]

    def carry(s, c, send_sem, peer):
        return pltpu.make_async_remote_copy(
            src_ref=piece(s, c),
            dst_ref=piece(s, c),
            send_sem=send_sem,
            recv_sem=recv.at[s, c],
            device_id={axis: peer},
            device_id_type=MESH,
        )

    def own_sends(c, action):
        for step in range(1, n):
            upward, downward = me + step < n, me >= step
            if n == 4 and step > 1:
                upward, downward = me + step < n - 1, me > step

            @pl.when(upward)
            def _():
                action(carry(me, c, send.at[c, step, 0], lax.rem(me + step, n)))

            @pl.when(downward)
            def _():
                action(carry(me, c, send.at[c, step, 1], lax.rem(me + n - step, n)))

    def middle_of(s):
        return (n - 2 if s < n // 2 else 1) if n == 4 else -1

    def relay(s, c):
        return carry(s, c, relay_send.at[s, c], 0 if s >= n // 2 else n - 1)

    def hand_on(s, c, due):
        @pl.when((me == middle_of(s)) & due)
        def _():
            relay(s, c).wait_recv()
            relay(s, c).start()

    def group(ref, g):
        return ref.at[pl.ds(g * (rows // GROUPS), rows // GROUPS)]

    def passing(way, k, g):
        peer = lax.rem(me + 1, n) if way == 0 else lax.rem(me + n - 1, n)
        return pltpu.make_async_remote_copy(
            src_ref=group(parts_ref.at[k], g),
            dst_ref=group(passed_ref.at[way, k], g),
            send_sem=sum_send.at[k, g],
            recv_sem=sum_recv.at[way, k, g],
            device_id={axis: peer},
            device_id_type=MESH,
        )

    def pass_on(way, k, joins):
        for g in range(GROUPS):
            span = pl.ds(g * (rows // GROUPS), rows // GROUPS)

            @pl.when(joins)
            def _():
                passing(way, k, g).wait_recv()
                parts_ref[k, span] = (
                    parts_ref[k, span].astype(F32) + passed_ref[way, k, span].astype(F32)
                ).astype(BF16)

            passing(way, k, g).start()

    def sum_step(c):
        k_up = c - me
        hops = n - 1 - me
        k_down = c - hops - jnp.minimum(hops, 1)

        @pl.when((k_up > me) & (k_up < n))
        def _():
            pass_on(0, k_up, me > 0)

        @pl.when((k_down >= 0) & (k_down < me))
        def _():
            pass_on(1, k_down, me < n - 1)

    for c in range(min(AHEAD, chunks)):
        own_sends(c, lambda copy: copy.start())
    order = sorted(range(n), key=lambda s: abs(2 * s - (n - 1)))

    for h in range(heads):
        state_ref[h] = jnp.zeros((DK, DK), F32)
    for load in loads:
        load.wait()
    experts = gate_in.shape[0]
    expert_loads = []
    for e in range(experts):
        pairs = ((gate_in, gate_ref), (up_in, up_ref), (down_in, down_ref))
        expert_loads.append(
            [
                pltpu.make_async_copy(source.at[e], target.at[e], expert_sem.at[e, i])
                for i, (source, target) in enumerate(pairs)
            ]
        )
        for load in expert_loads[e]:
            load.start()

    capacity, model_width = outgoing_ref.shape[2:]
    experts_total = router_ref.shape[0]
    slots = experts_total * capacity
    sub, lane = (lax.broadcasted_iota(jnp.int32, (rows, rows), i) for i in (0, 1))
    label = lax.broadcasted_iota(jnp.int32, (rows, experts_total), 1)
    base = ((label % experts) * (owners * capacity) + (label // experts) * capacity).astype(F32)

    def choose(k):
        named = jnp.where(sub == lane, ids_ref[k : k + 1, :].astype(F32), 0.0)
        return jnp.sum(named, -1, keepdims=True) == label.astype(F32)

    picks = sum(choose(k).astype(F32) for k in range(2))
    earlier = dot1((sub > lane).astype(F32), picks)
    slot = lax.broadcasted_iota(jnp.int32, (rows, slots), 1).astype(F32)
    for k in range(2):
        target = jnp.sum(jnp.where(choose(k), earlier + base, 0.0), -1, keepdims=True)
        placed_ref[k] = (slot == target).astype(F32)

    rows_c = NH * CT
    later = lax.broadcasted_iota(jnp.int32, (rows_c, rows_c), 0)
    early = lax.broadcasted_iota(jnp.int32, (rows_c, rows_c), 1)
    later_t, early_t = later % CT, early % CT
    same_token = later_t == early_t
    strict = (early_t < later_t) | (same_token & (early < later))
    eye = (later == early).astype(F32)
    seen = (lax.broadcasted_iota(jnp.int32, (CT, rows_c), 1) % CT) <= lax.broadcasted_iota(
        jnp.int32, (CT, rows_c), 0
    )

    def unit(values):
        return values * lax.rsqrt(jnp.sum(values * values, -1, keepdims=True) + EPSILON)

    def head_of(values, h):
        return values[:, h * DK : (h + 1) * DK]

    def step_chunk(c, _):
        if AHEAD < chunks:

            @pl.when(c + AHEAD < chunks)
            def _():
                own_sends(c + AHEAD, lambda copy: copy.start())

        if n == 4:
            for s in order:
                hand_on(s, c, c == 0)
            for s in order:
                hand_on(s, c + 1, c + 1 < chunks)
        for s in order:

            @pl.when((me != s) & (me != middle_of(s)))
            def _():
                carry(s, c, send.at[0, 0, 0], lax.rem(me + 1, n)).wait_recv()

        span = pl.ds(pl.multiple_of(c * rows, rows), rows)
        square = jnp.zeros((rows, 1), F32)
        for s in range(n):
            part = blocks_ref[s, span].astype(F32)
            square = square + jnp.sum(part * part, -1, keepdims=True)
        scale = lax.rsqrt(square / (n * width) + EPSILON)
        for s in range(n):
            cols = pl.ds(s * width, width)
            normed_ref[:, cols] = (
                blocks_ref[s, span].astype(F32) * scale * gain_ref[:, cols]
            ).astype(BF16)

        def project(weight):
            return jnp.dot(normed_ref[...], weight, preferred_element_type=F32)

        key_parts = [project(kw_ref[m]) for m in range(NH)]
        beta = 2.0 / (
            1.0
            + jnp.exp(
                -lax.dot_general(normed_ref[...], bw_ref[...], NT, preferred_element_type=F32)
            )
        )

        def rows_of(member_parts, j):
            return jnp.concatenate(
                [part[j * CT : (j + 1) * CT] for part in member_parts], 0
            )

        cases = [(h, j) for h in range(heads) for j in range(subs)]
        units = [[unit(head_of(part, h)) for part in key_parts] for h in range(heads)]
        all_keys, all_scaled, betas, parts = [], [], [], []
        for h, j in cases:
            keys = rows_of(units[h], j)
            betas.append(
                rows_of([beta[:, h * NH + m : h * NH + m + 1] for m in range(NH)], j)
            )
            scaled = keys * betas[-1]
            all_scaled.append(scaled)
            all_keys.append(halves(keys))
            similar = dot3(halves(scaled), all_keys[-1], NT)
            parts.append(jnp.where(strict, similar, 0.0))
        inverses = []
        for part in parts:
            inner = jnp.where(same_token, part, 0.0)
            inverses.append(eye - inner + dot1(inner, inner))
        side = [lambda m=m: project(vw_ref[m]) for m in range(NH)]
        side.append(lambda: project(qw_ref[...]))
        side_parts = []
        size = 1
        while size < CT:
            joined = (later_t // (2 * size) == early_t // (2 * size)) & (
                later_t // size != early_t // size
            )
            steps = [
                dot1(jnp.where(joined, part, 0.0), inverse)
                for part, inverse in zip(parts, inverses)
            ]
            if side:
                side_parts.append(side.pop(0)())
            inverses = [
                inverse - dot1(inverse, step) for inverse, step in zip(inverses, steps)
            ]
            size *= 2
        while side:
            side_parts.append(side.pop(0)())
        value_parts, query_part = side_parts[:NH], side_parts[NH]
        queries = [
            halves(unit(head_of(query_part, h))[j * CT : (j + 1) * CT] * DK ** (-0.5))
            for h, j in cases
        ]
        rights = [
            jnp.concatenate(
                [scaled, rows_of([head_of(part, h) for part in value_parts], j) * betas_now], 1
            )
            for (h, j), scaled, betas_now in zip(cases, all_scaled, betas)
        ]
        guesses = [dot1(inverse, right) for inverse, right in zip(inverses, rights)]
        attends = [
            halves(jnp.where(seen, dot3(query, keys, NT), 0.0))
            for query, keys in zip(queries, all_keys)
        ]
        rests = [
            right - guess - dot3(halves(part), halves(guess))
            for right, guess, part in zip(rights, guesses, parts)
        ]
        all_solved = [
            guess + dot1(inverse, rest)
            for guess, inverse, rest in zip(guesses, inverses, rests)
        ]
        befores = [state_ref[h] for h in range(heads)]
        mixes = [[] for _ in range(heads)]
        for j in range(subs):
            for h in range(heads):
                i = h * subs + j
                state = halves(befores[h])
                solved = all_solved[i]
                corrected = solved[:, DK:] - dot3(halves(solved[:, :DK]), state)
                split = halves(corrected)
                mixed = dot3(queries[i], state) + dot3(attends[i], split)
                befores[h] = befores[h] + dot3(all_keys[i], split, TN)
                mixes[h].append(root_norm(mixed, head_gain_ref[...]).astype(BF16))
        for h in range(heads):
            state_ref[h] = befores[h]
        mixes = [jnp.concatenate(mix, 0) for mix in mixes]
        parts_ref[c] = jnp.dot(
            jnp.concatenate(mixes, 1), ow_ref[...], preferred_element_type=F32
        ).astype(BF16)
        sum_step(c)
        return 0

    lax.fori_loop(0, chunks, step_chunk, 0)
    for c in range(chunks, 2 * n):
        sum_step(c)
    mine = pl.ds(pl.multiple_of(me * rows, rows), rows)
    for s in range(n):
        cols = pl.ds(s * width, width)
        residual_ref[:, cols] = blocks_ref[s, mine].astype(F32) + parts_ref[me, :, cols].astype(F32)
    for way, comes in ((0, me > 0), (1, me < n - 1)):
        for g in range(GROUPS):
            span = pl.ds(g * (rows // GROUPS), rows // GROUPS)

            @pl.when(comes)
            def _():
                passing(way, me, g).wait_recv()
                residual_ref[span] += passed_ref[way, me, span].astype(F32)

    residual = residual_ref[...]
    routed = root_norm(residual, expert_gain_ref[...])
    spread = (placed_ref[0] + placed_ref[1]).astype(BF16)
    expert_rows = routed.astype(BF16)
    copies, keeps = [], []

    def across(source, target, sends, receives, e, step):
        return pltpu.make_async_remote_copy(
            src_ref=source.at[e, peers[step]],
            dst_ref=target.at[e, this],
            send_sem=sends.at[e, step],
            recv_sem=receives.at[e, step],
            device_id={owners_axis: peers[step]},
            device_id_type=MESH,
        )

    def keep(source, target, i, e):
        keeps.append(
            pltpu.make_async_copy(source.at[e, this], target.at[e, this], keep_sem.at[i, e])
        )
        keeps[-1].start()
        return keeps[-1]

    kept = []
    for e in range(experts):
        here = spread[:, e * owners * capacity : (e + 1) * owners * capacity]
        outgoing = lax.dot_general(
            here, expert_rows, TN, preferred_element_type=F32
        ).astype(BF16)
        for s in range(owners):
            outgoing_ref[e, s] = outgoing[s * capacity : (s + 1) * capacity]
        copies.append([])
        for step in steps:
            copies[e].append(
                across(outgoing_ref, arrived_ref, there_send, there_recv, e, step)
            )
            copies[e][-1].start()
        kept.append(keep(outgoing_ref, arrived_ref, 0, e))
    logits = lax.dot_general(
        routed, router_ref[...], NT, precision=TOP_PRECISION, preferred_element_type=F32
    )
    chosen = [jnp.sum(jnp.where(choose(k), logits, 0.0), -1, keepdims=True) for k in range(2)]
    leading = 1.0 / (1.0 + jnp.exp(chosen[1] - chosen[0]))
    weights = placed_ref[0] * leading + placed_ref[1] * (1.0 - leading)
    stacked = jnp.concatenate(halves(weights), 0)
    returns = []
    for e in range(experts):
        for copy in copies[e]:
            copy.wait_recv()
        kept[e].wait()
        arrived = jnp.concatenate([arrived_ref[e, s] for s in range(owners)], 0)
        expert_loads[e][0].wait()
        gated = jnp.dot(arrived, gate_ref[e], preferred_element_type=F32)
        expert_loads[e][1].wait()
        lifted = jnp.dot(arrived, up_ref[e], preferred_element_type=F32)
        hidden = (gated / (1.0 + jnp.exp(-gated)) * lifted).astype(BF16)
        expert_loads[e][2].wait()
        made = jnp.dot(hidden, down_ref[e], preferred_element_type=F32).astype(BF16)
        for s in range(owners):
            result_ref[e, s] = made[s * capacity : (s + 1) * capacity]
        returns.append([])
        for step in steps:
            returns[e].append(across(result_ref, back_ref, back_send, back_recv, e, step))
            returns[e][-1].start()
        kept.append(keep(result_ref, back_ref, 1, e))
    blended = residual_ref[...]
    for e in range(experts):
        for copy in returns[e]:
            copy.wait_recv()
        kept[experts + e].wait()
        back = jnp.concatenate([back_ref[e, s] for s in range(owners)], 0)
        share = stacked[:, e * owners * capacity : (e + 1) * owners * capacity]
        both = jnp.dot(share, back, preferred_element_type=F32)
        blended = blended + (both[:rows] + both[rows:])
    out_ref[...] = blended.astype(BF16)
    for copy in sum(copies + returns, []):
        copy.wait_send()

    for c in range(n):

        @pl.when(me != c)
        def _():
            for g in range(GROUPS):
                passing(0, c, g).wait_send()

    for c in range(chunks):
        own_sends(c, lambda copy: copy.wait_send())
        if n == 4:
            for s in range(n):

                @pl.when(me == middle_of(s))
                def _():
                    relay(s, c).wait_send()


def layer(axis, n, owners_axis, owners, x, *arrays):
    length, width = x.shape
    qw, kw, vw, bw, head_gain, ow, expert_gain, router, ids, gate, up, down = arrays[1:]
    heads = qw.shape[1] // DK
    model_width = n * width
    chunks, rows = n, length // n
    experts = gate.shape[0]
    capacity = 4 * rows // router.shape[1]
    gain, head_gain, expert_gain = (
        values.reshape(1, -1) for values in (arrays[0], head_gain, expert_gain)
    )
    small = (gain, qw, kw, vw, bw.T, head_gain, ow, ids.T, expert_gain, router.T)
    slotted = pltpu.VMEM((experts, owners, capacity, model_width), BF16)
    peer_sems = pltpu.SemaphoreType.DMA((experts, owners))
    return pl.pallas_call(
        functools.partial(layer_kernel, axis, n, heads, owners_axis, owners),
        out_shape=jax.ShapeDtypeStruct((rows, model_width), BF16),
        in_specs=[ANY] * 14,
        out_specs=VMEM,
        scratch_shapes=[
            pltpu.VMEM((n, length, width), BF16),
            pltpu.VMEM((rows, model_width), BF16),
            pltpu.VMEM((chunks, rows, model_width), BF16),
            pltpu.VMEM((2, chunks, rows, model_width), BF16),
            pltpu.VMEM((heads, DK, DK), F32),
            pltpu.VMEM((rows, model_width), F32),
            pltpu.VMEM((2, rows, router.shape[1] * capacity), F32),
        ]
        + [pltpu.VMEM(array.shape, array.dtype) for array in small + (gate, up, down)]
        + [slotted] * 4
        + [
            pltpu.SemaphoreType.DMA((len(small),)),
            pltpu.SemaphoreType.DMA,
            pltpu.SemaphoreType.DMA((chunks, n, 2)),
            pltpu.SemaphoreType.DMA((n, chunks)),
            pltpu.SemaphoreType.DMA((n, chunks)),
            pltpu.SemaphoreType.DMA((chunks, GROUPS)),
            pltpu.SemaphoreType.DMA((2, chunks, GROUPS)),
            pltpu.SemaphoreType.DMA((experts, 3)),
            peer_sems,
            peer_sems,
            peer_sems,
            peer_sems,
            pltpu.SemaphoreType.DMA((2, experts)),
        ],
        compiler_params=pltpu.CompilerParams(
            collective_id=0, has_side_effects=True, vmem_limit_bytes=63 << 20
        ),
        cost_estimate=pl.CostEstimate(
            flops=20 << 30, bytes_accessed=50 << 20, transcendentals=0
        ),
        name="layer",
    )(x, *small, gate, up, down)


def shards(heads_axis, owners, *arrays):
    return layer("head", heads_axis, "dp", owners, *arrays)


def solution(mesh):
    return jax.shard_map(
        functools.partial(shards, mesh.shape["head"], mesh.shape["dp"]),
        mesh=mesh,
        in_specs=(
            P("dp", "head"),
            P(),
            P(None, "head"),
            P(None, None, "head"),
            P(None, None, "head"),
            P(None, "head"),
            P(),
            P("head", None),
            P(),
            P(),
            P(("dp", "head"), None),
            P("dp", None, None),
            P("dp", None, None),
            P("dp", None, None),
        ),
        out_specs=P(("dp", "head"), None),
        check_vma=False,
    )
```
